512 devices in a mesh: blk: 32 (over x, z), batch: 16 (over y, core).
Axes of the slice: x: 4, y: 8, z: 8, core: 2. Of those that a mesh axis runs over, the one named last changes fastest.
Arguments:
- queries: bfloat16 [16, 8192, 2048], P('batch', 'blk'), may hold values from -8 to 8
- keys: bfloat16 [16, 8192, 1024], P('batch', 'blk'), may hold values from -8 to 8
- values: bfloat16 [16, 8192, 1024], P('batch', 'blk'), may hold values from -6 to 6
- seg_ids: int32 [16, 8192], P('batch', 'blk'), may hold values from 0 to 6, as said below
- lengths: int32 [16, 7], P('batch'), may hold values from 128 to 2048, as said below
- live: int32 [16, 32, 8], P('batch', 'blk'), may hold values from 0 to 1, as said below
- page_table: int32 [16, 7, 2], replicated, may hold values from 0 to 127, as said below
- pool: bfloat16 [128, 16, 2048], P('batch'), may hold values from -6 to 6
Outputs:
- attended: bfloat16 [16, 8192, 2048], P('batch', 'blk')
- cache_keys: bfloat16 [16, 8192, 1024], P('batch', 'blk')
The draws below stay inside these ranges and needn't reach their ends.
Inputs may be any that keep to these rules, and one draw needn't show every extreme that they name: Each stream's lengths sum to 8192; one of them is exactly 2048, three lie between 1536 and 1920, and three between 128 and 512, in random order. seg_ids[b, t] is the prompt that token t falls in under lengths[b]: it never decreases and every prompt number appears. live[b, j, r - 1] is 1 exactly when j >= r and the first token of block j and the last token of block j - r have the same seg_ids. `page_table`: page p is held by index p // 8 of batch. Of one stream's 7 * 2 pages, at most 2 are held by any one index of batch, and exactly 2 by one of them in every stream.
All inputs are finite; a program needn't handle non-finite values.
Results may differ from the reference program's by a relative error of at most 0.0055.
The reference program's roundings to bfloat16 on the way count: a program that leaves them out, or rounds other values in their place, can miss the bound.
Values may be sent and summed in bfloat16 or wider, within the bound.
A program may use at most 128 MiB of HBM per device.

```python
import math
import jax
import jax.numpy as jnp
from jax import lax

QUERY_HEADS = 16
KEY_VALUE_HEADS = 8
HEAD_SIZE = 128
BLOCK_TOKENS = 256
SEGS = 7
PAGE = 16
PAGES_SEG = 2
POOL_DEV = 8
KVW = 1024
PACKED_STREAMS = 16
STREAM_TOKENS = 8192
STEPS = 8
LONG = 2048
PAGES = 128
CAP = 2
N_BLK = 32


def layout(key):
    short_key, order_key = jax.random.split(key)
    shorts = jax.random.randint(short_key, (PACKED_STREAMS, 3), LONG // 16, LONG // 4 + 1)
    seg_lengths = jnp.concatenate([jnp.full((PACKED_STREAMS, 1), LONG, jnp.int32), LONG - shorts, shorts], axis=1).astype(jnp.int32)
    orders = jax.vmap(lambda one_key: jax.random.permutation(one_key, SEGS))(jax.random.split(order_key, PACKED_STREAMS))
    seg_lengths = jnp.take_along_axis(seg_lengths, orders, axis=1).astype(jnp.int32)
    seg_ends = jnp.cumsum(seg_lengths, axis=1)
    token_index = jnp.arange(STREAM_TOKENS, dtype=jnp.int32)
    segment = jnp.sum((seg_ends[:, None, :] <= token_index[None, :, None]).astype(jnp.int32), axis=2).astype(jnp.int32)
    return (seg_lengths, segment)


def draw_lengths(key, part):
    return layout(jax.random.fold_in(key, 17))[0]


def draw_seg_ids(key, part):
    return layout(jax.random.fold_in(key, 17))[1]


def draw_live(key, part):
    segment = layout(jax.random.fold_in(key, 17))[1]
    block_total = STREAM_TOKENS // BLOCK_TOKENS
    blocks = segment.reshape(PACKED_STREAMS, block_total, BLOCK_TOKENS)
    first_seg = blocks[:, :, 0]
    last_seg = blocks[:, :, BLOCK_TOKENS - 1]
    distance = jnp.arange(1, STEPS + 1, dtype=jnp.int32)
    earlier = jnp.arange(block_total, dtype=jnp.int32)[:, None] - distance[None, :]
    earlier_last = jnp.take(last_seg, jnp.clip(earlier, 0, block_total - 1), axis=1)
    return ((earlier[None] >= 0) & (earlier_last == first_seg[:, :, None])).astype(jnp.int32)


def draw_page_table(key, part):
    page_total = SEGS * PAGES_SEG

    def one_stream(stream_key):
        key_one, key_two, key_three, key_four = jax.random.split(stream_key, 4)
        heavy = jax.random.randint(key_one, (), 0, PACKED_STREAMS)
        others = jnp.arange((PACKED_STREAMS - 1) * CAP, dtype=jnp.int32) // CAP
        others = others + (others >= heavy).astype(jnp.int32)
        others = jax.random.permutation(key_two, others)[:page_total - CAP]
        holders = jnp.concatenate([jnp.full((CAP,), heavy, jnp.int32), others])
        holders = jax.random.permutation(key_three, holders)
        inside = jax.random.randint(key_four, (page_total,), 0, POOL_DEV)
        return (holders * POOL_DEV + inside).reshape(SEGS, PAGES_SEG)
    return jax.vmap(one_stream)(jax.random.split(jax.random.fold_in(key, 29), PACKED_STREAMS)).astype(jnp.int32)


def base_field(key, tensor_shape):
    return jnp.clip(jax.random.normal(key, tensor_shape, jnp.float32), -8.0, 8.0)


def draw_queries(key, part):
    tensor_shape = (PACKED_STREAMS, STREAM_TOKENS, QUERY_HEADS * HEAD_SIZE)
    field = base_field(jax.random.fold_in(key, 41), tensor_shape)
    return field.astype(jnp.bfloat16)


def draw_keys(key, part):
    tensor_shape = (PACKED_STREAMS, STREAM_TOKENS, KEY_VALUE_HEADS * HEAD_SIZE)
    field = base_field(jax.random.fold_in(key, 43), tensor_shape)
    return field.astype(jnp.bfloat16)


def levels(key, dims, cuts, low, top_value):
    def one(axis_at, shards_of):
        heights = jax.random.uniform(jax.random.fold_in(jax.random.fold_in(key, 6), axis_at), (shards_of,), jnp.float32, low / len(cuts), top_value / len(cuts))
        return jnp.repeat(jnp.exp(heights), dims[axis_at] // shards_of).reshape((-1,) + (1,) * (len(dims) - axis_at - 1))

    loudness = one(*cuts[0])
    for cut in cuts[1:]:
        loudness = loudness * one(*cut)
    return loudness


def gaussian(rng, shape, scale, most, cuts=(), kind=jnp.bfloat16):
    values = scale * jax.random.normal(rng, shape, jnp.float32)
    if cuts:
        values = values * levels(rng, shape, cuts, -0.22, 0.18)
    return jnp.clip(values, -most, most).astype(kind)


def setup_inputs(seed: int = 0) -> dict:
    key_of = jax.random.split(jax.random.key(seed), 9)
    queries = draw_queries(jax.random.fold_in(key_of[8], 71), 0)
    keys = draw_keys(jax.random.fold_in(key_of[8], 71), 0)
    values = gaussian(key_of[2], (PACKED_STREAMS, STREAM_TOKENS, KVW), 1.0, 6.0, ((0, 16), (1, 32)))
    seg_ids = draw_seg_ids(jax.random.fold_in(key_of[8], 71), 0)
    lengths = draw_lengths(jax.random.fold_in(key_of[8], 71), 0)
    live = draw_live(jax.random.fold_in(key_of[8], 71), 0)
    page_table = draw_page_table(jax.random.fold_in(key_of[8], 71), 0)
    pool = gaussian(key_of[7], (PAGES, PAGE, 2 * KVW), 1.0, 6.0, ((0, 16),))
    return dict(queries=queries, keys=keys, values=values, seg_ids=seg_ids, lengths=lengths, live=live, page_table=page_table, pool=pool)


rope_base = 1000000.0

def apply_rotary(matrix, token_position, head_count):
    head_width = matrix.shape[-1] // head_count
    halfway = head_width // 2
    inverse = jnp.power(jnp.float32(rope_base), -2.0 * jnp.arange(halfway, dtype=jnp.float32) / head_width)
    angles = token_position.astype(jnp.float32)[:, None] * inverse[None, :]
    cosine = jnp.cos(angles)[:, None, :]
    sine_part = jnp.sin(angles)[:, None, :]
    split_heads = matrix.astype(jnp.float32).reshape(matrix.shape[0], head_count, head_width)
    leading = split_heads[..., :halfway]
    trailing = split_heads[..., halfway:]
    turned = jnp.concatenate([leading * cosine - trailing * sine_part, trailing * cosine + leading * sine_part], axis=-1)
    return turned.reshape(matrix.shape[0], head_count * head_width).astype(jnp.bfloat16)

def segment_of(indices, lengths):
    seg_ends = jnp.cumsum(lengths).astype(jnp.int32)
    return lax.optimization_barrier(jnp.sum((seg_ends[None, :] <= indices[:, None]).astype(jnp.int32), axis=1)).astype(jnp.int32)

def positions(segment, lengths, offset, prefix_len):
    starts = (jnp.cumsum(lengths) - lengths).astype(jnp.int32)
    labels = jnp.arange(lengths.shape[0], dtype=jnp.int32)
    own_start = lax.optimization_barrier(jnp.sum(jnp.where(segment[:, None] == labels[None, :], starts[None, :], 0), axis=1)).astype(jnp.int32)
    token_index = (offset + jnp.arange(segment.shape[0], dtype=jnp.int32)).astype(jnp.int32)
    return (prefix_len + token_index - own_start).astype(jnp.int32)

def reference(queries, keys, values, seg_ids, lengths, live, page_table, pool):
    stream_len = queries.shape[1]
    q_width = queries.shape[2]
    kv_width = keys.shape[2]
    query_groups = QUERY_HEADS // KEY_VALUE_HEADS
    prefix_len = PAGES_SEG * PAGE
    scaling = 1.0 / math.sqrt(HEAD_SIZE)
    span = (STEPS + 1) * BLOCK_TOKENS

    def one_stream(stream_index):
        segment = seg_ids[stream_index]
        own_lengths = lengths[stream_index]
        token_position = positions(segment, own_lengths, 0, prefix_len)
        query_rotated = apply_rotary(queries[stream_index], token_position, QUERY_HEADS)
        key_rotated = apply_rotary(keys[stream_index], token_position, KEY_VALUE_HEADS)
        page_list = page_table[stream_index].reshape(-1)
        prefix = pool[page_list].reshape(SEGS * prefix_len, 2 * kv_width)
        pre_keys = prefix[:, :kv_width]
        pre_values = prefix[:, kv_width:]
        pre_seg = (jnp.arange(SEGS * prefix_len, dtype=jnp.int32) // prefix_len).astype(jnp.int32)
        padded_keys = jnp.concatenate([jnp.zeros((STEPS * BLOCK_TOKENS, kv_width), jnp.bfloat16), key_rotated], axis=0)
        padded_values = jnp.concatenate([jnp.zeros((STEPS * BLOCK_TOKENS, kv_width), jnp.bfloat16), values[stream_index]], axis=0)
        live_rows = live[stream_index]

        def one_block(block_id):
            start = (block_id * BLOCK_TOKENS).astype(jnp.int32)
            query_block = lax.dynamic_slice_in_dim(query_rotated, start, BLOCK_TOKENS, 0)
            query_seg = lax.dynamic_slice_in_dim(segment, start, BLOCK_TOKENS, 0)
            query_idx = (start + jnp.arange(BLOCK_TOKENS, dtype=jnp.int32)).astype(jnp.int32)
            window_keys = lax.dynamic_slice_in_dim(padded_keys, start, span, 0)
            window_values = lax.dynamic_slice_in_dim(padded_values, start, span, 0)
            key_idx = ((block_id - STEPS) * BLOCK_TOKENS + jnp.arange(span, dtype=jnp.int32)).astype(jnp.int32)
            key_seg = segment_of(key_idx, own_lengths)
            block_live = jnp.concatenate([live_rows[block_id][::-1], jnp.ones((1,), jnp.int32)]).astype(jnp.int32)
            key_live = jnp.repeat(block_live, BLOCK_TOKENS)
            seen_pre = query_seg[:, None] == pre_seg[None, :]
            seen_win = (query_seg[:, None] == key_seg[None, :]) & (key_idx[None, :] <= query_idx[:, None])
            seen_win = seen_win & (key_idx[None, :] >= 0) & (key_live[None, :] > 0)
            seen = jnp.concatenate([seen_pre, seen_win], axis=1)
            joined_keys = jnp.concatenate([pre_keys, window_keys], axis=0)
            joined_values = jnp.concatenate([pre_values, window_values], axis=0)
            query_heads = query_block.astype(jnp.float32).reshape(BLOCK_TOKENS, KEY_VALUE_HEADS, query_groups, HEAD_SIZE)
            key_heads = joined_keys.astype(jnp.float32).reshape(-1, KEY_VALUE_HEADS, HEAD_SIZE)
            value_heads = joined_values.astype(jnp.float32).reshape(-1, KEY_VALUE_HEADS, HEAD_SIZE)
            score = jnp.einsum('thgd,uhd->hgtu', query_heads, key_heads) * scaling
            score = jnp.where(seen[None, None], score, -jnp.inf)
            highest = lax.optimization_barrier(jnp.max(score, axis=-1, keepdims=True))
            weight = jnp.exp(score - highest)
            total = lax.optimization_barrier(jnp.sum(weight, axis=-1))
            rounded = lax.optimization_barrier(weight.astype(jnp.bfloat16)).astype(jnp.float32)
            summed = jnp.einsum('hgtu,uhd->thgd', rounded, value_heads)
            result = summed / jnp.transpose(total, (2, 0, 1))[..., None]
            return result.reshape(BLOCK_TOKENS, q_width).astype(jnp.bfloat16)
        blocks = lax.map(one_block, jnp.arange(N_BLK, dtype=jnp.int32))
        return (blocks.reshape(stream_len, q_width), key_rotated)
    attended, cache_keys = lax.map(one_stream, jnp.arange(queries.shape[0], dtype=jnp.int32))
    return (attended, cache_keys)
```

```python
import math

import jax
import jax.numpy as jnp
import numpy as np
from jax import lax
from jax.experimental import pallas as pl
from jax.experimental.pallas import tpu as pltpu
from jax.sharding import PartitionSpec as P

HEAD = 128
KV_HEADS = 8
RING = 8
TOK = 256
SEGS = 7
PAGES_SEG = 2
PAGE = 16
PREFIX = PAGES_SEG * PAGE
PAIR = 2 * HEAD
ROPE_BASE = 1000000.0
LOG2E_SCALE = math.log2(math.e) / math.sqrt(HEAD)
NEG = -1e30
MESH = pl.DeviceIdType.MESH


def kernel(
    n_x,
    n_batch,
    pool_rows,
    queries,
    keys,
    values,
    lengths,
    page_table,
    pool,
    freq,
    attended,
    cache,
    qrot,
    krot,
    qbuf,
    kvbuf,
    pbuf,
    pown,
    pre,
    scores,
    q2,
    obuf,
    v_send,
    v_recv,
    k_send,
    k_recv,
    q_send,
    q_recv,
    f_send,
    f_recv,
    p_send,
    p_recv,
    o_send,
    o_recv,
    local,
):
    blk = lax.axis_index("blk")
    bat = lax.axis_index("batch")
    z = lax.rem(blk, RING)
    x = lax.div(blk, RING)

    def ring(d):
        return lax.rem(z + d, RING)

    def ring_id(d):
        return (x * RING + ring(d), bat)

    def other(e):
        return lax.rem(bat + e, n_batch)

    def lanes(i, width):
        return pl.ds(pl.multiple_of(i * width, width), width)

    def rows(i):
        return pl.ds(pl.multiple_of(i * TOK, TOK), TOK)

    ahead = (lax.rem(x + 1, n_x) * RING + z, bat)
    behind = (lax.rem(x + n_x - 1, n_x) * RING + z, bat)

    barrier = pltpu.get_barrier_semaphore()
    for d in range(1, RING):
        pl.semaphore_signal(barrier, inc=1, device_id=ring_id(d), device_id_type=MESH)
    for who in (ahead, behind):
        pl.semaphore_signal(barrier, inc=1, device_id=who, device_id_type=MESH)
    for e in range(1, n_batch):
        pl.semaphore_signal(barrier, inc=1, device_id=(blk, other(e)), device_id_type=MESH)
    own_pool_k = pltpu.make_async_copy(pool.at[:, :, lanes(z, HEAD)], pown.at[:, :, 0:HEAD], local.at[0])
    own_pool_v = pltpu.make_async_copy(
        pool.at[:, :, lanes(z + KV_HEADS, HEAD)], pown.at[:, :, HEAD:PAIR], local.at[1]
    )
    own_v = pltpu.make_async_copy(
        values.at[0, :, lanes(z, HEAD)], kvbuf.at[rows(RING + z), HEAD:PAIR], local.at[2]
    )
    own_pool_k.start()
    own_pool_v.start()
    own_v.start()
    pl.semaphore_wait(barrier, RING - 1 + 2 + n_batch - 1)

    def send_v(d):
        return pltpu.make_async_remote_copy(
            src_ref=values.at[0, :, lanes(ring(d), HEAD)],
            dst_ref=kvbuf.at[rows(RING + z), HEAD:PAIR],
            send_sem=v_send.at[d],
            recv_sem=v_recv.at[d],
            device_id=ring_id(d),
            device_id_type=MESH,
        )

    def send_k(d):
        return pltpu.make_async_remote_copy(
            src_ref=krot.at[:, lanes(ring(d), HEAD)],
            dst_ref=kvbuf.at[rows(RING + z), 0:HEAD],
            send_sem=k_send.at[d],
            recv_sem=k_recv.at[d],
            device_id=ring_id(d),
            device_id_type=MESH,
        )

    def send_q(d):
        return pltpu.make_async_remote_copy(
            src_ref=qrot.at[:, lanes(ring(d), PAIR)],
            dst_ref=qbuf.at[z],
            send_sem=q_send.at[d],
            recv_sem=q_recv.at[d],
            device_id=ring_id(d),
            device_id_type=MESH,
        )

    def send_pool(e):
        return pltpu.make_async_remote_copy(
            src_ref=pown,
            dst_ref=pbuf.at[pl.ds(bat * pool_rows, pool_rows)],
            send_sem=p_send.at[e],
            recv_sem=p_recv.at[e],
            device_id=(blk, other(e)),
            device_id_type=MESH,
        )

    def forward(s):
        return pltpu.make_async_remote_copy(
            src_ref=kvbuf.at[rows(RING + s)],
            dst_ref=kvbuf.at[rows(s)],
            send_sem=f_send.at[s],
            recv_sem=f_recv.at[s],
            device_id=ahead,
            device_id_type=MESH,
        )

    def send_o(d):
        return pltpu.make_async_remote_copy(
            src_ref=obuf.at[d],
            dst_ref=attended.at[0, :, lanes(z, PAIR)],
            send_sem=o_send.at[d],
            recv_sem=o_recv.at[d],
            device_id=ring_id(RING - d),
            device_id_type=MESH,
        )

    near = (1, 7, 2, 6, 3, 5, 4)
    for d in near:
        send_v(d).start()
    own_pool_k.wait()
    own_pool_v.wait()
    for e in range(1, n_batch):
        send_pool(e).start()
    own_pool = pltpu.make_async_copy(pown, pbuf.at[pl.ds(bat * pool_rows, pool_rows)], local.at[0])
    own_pool.start()

    starts = [jnp.int32(0)]
    for s in range(SEGS - 1):
        starts.append(starts[-1] + lengths[0, s])

    def start_and_segment(token):
        first = jnp.zeros_like(token)
        segment = jnp.zeros_like(token)
        for s in range(1, SEGS):
            inside = token >= starts[s]
            first = jnp.where(inside, starts[s], first)
            segment = jnp.where(inside, s, segment)
        return first, segment

    row = lax.broadcasted_iota(jnp.int32, (TOK, HEAD), 0)
    lane = lax.broadcasted_iota(jnp.int32, (TOK, HEAD), 1)
    token = row + blk * TOK
    first, _ = start_and_segment(token)
    angle = (PREFIX + token - first).astype(jnp.float32) * freq[0:1, :]
    cosine = jnp.cos(angle)
    sine = jnp.sin(angle)
    sine = jnp.where(lane < HEAD // 2, -sine, sine)

    def turn(part):
        part = part.astype(jnp.float32)
        return (part * cosine + pltpu.roll(part, HEAD // 2, 1) * sine).astype(jnp.bfloat16)

    for h in range(KV_HEADS):
        krot[:, h * HEAD : (h + 1) * HEAD] = turn(keys[0, :, h * HEAD : (h + 1) * HEAD])
    for d in near:
        send_k(d).start()
    own_k = pltpu.make_async_copy(
        krot.at[:, lanes(z, HEAD)], kvbuf.at[rows(RING + z), 0:HEAD], local.at[1]
    )
    own_k.start()
    cache_copy = pltpu.make_async_copy(krot, cache.at[0], local.at[3])
    cache_copy.start()
    for h in range(2 * KV_HEADS):
        qrot[:, h * HEAD : (h + 1) * HEAD] = turn(queries[0, :, h * HEAD : (h + 1) * HEAD])
    for d in near:
        send_q(d).start()
    own_q = pltpu.make_async_copy(qrot.at[:, lanes(z, PAIR)], qbuf.at[z], local.at[4])
    own_q.start()

    own_v.wait()
    own_k.wait()
    forward(z).start()

    def from_ring(sem, width_lo, d):
        src = ring(RING - d)
        view = kvbuf.at[rows(RING + src), width_lo : width_lo + HEAD]
        return pltpu.make_async_remote_copy(
            src_ref=view,
            dst_ref=view,
            send_sem=v_send.at[d],
            recv_sem=sem.at[d],
            device_id=ring_id(RING - d),
            device_id_type=MESH,
        )

    for d in near:
        from_ring(v_recv, HEAD, d).wait_recv()
        from_ring(k_recv, 0, d).wait_recv()
        forward(ring(RING - d)).start()

    own_pool.wait()
    for e in range(1, n_batch):
        src = pl.ds(lax.rem(bat + n_batch - e, n_batch) * pool_rows, pool_rows)
        pltpu.make_async_remote_copy(
            src_ref=pown,
            dst_ref=pbuf.at[src],
            send_sem=p_send.at[e],
            recv_sem=p_recv.at[e],
            device_id=(blk, other(n_batch - e)),
            device_id_type=MESH,
        ).wait_recv()
    for s in range(SEGS):
        for i in range(PAGES_SEG):
            at = s * PREFIX + i * PAGE
            pre[at : at + PAGE, :] = pbuf[page_table[bat, s, i]]
    pre[SEGS * PREFIX :, :] = jnp.zeros((TOK - SEGS * PREFIX, PAIR), jnp.bfloat16)

    for s in range(RING):
        forward(s).wait_recv()

    row2 = lax.rem(lax.broadcasted_iota(jnp.int32, (2 * TOK, HEAD), 0), TOK)
    lane2 = lax.broadcasted_iota(jnp.int32, (2 * TOK, HEAD), 1)
    contract_last = (((1,), (1,)), ((), ()))

    def one_block(i, carry):
        odd = lax.rem(i, 2)
        half = lax.div(i + 1, 2)
        d = lax.rem(odd * half + (1 - odd) * (RING - half), RING)
        src = ring(RING - d)

        @pl.when(i == 0)
        def _():
            pltpu.make_async_copy(qrot.at[:, lanes(z, PAIR)], qbuf.at[z], local.at[4]).wait()

        @pl.when(i > 0)
        def _():
            pltpu.make_async_remote_copy(
                src_ref=qbuf.at[src],
                dst_ref=qbuf.at[src],
                send_sem=q_send.at[d],
                recv_sem=q_recv.at[d],
                device_id=ring_id(RING - d),
                device_id_type=MESH,
            ).wait_recv()

        q2[0:TOK, :] = qbuf[src, :, 0:HEAD]
        q2[TOK : 2 * TOK, :] = qbuf[src, :, HEAD:PAIR]
        block0 = (x * RING + src) * TOK
        begin, segment = start_and_segment(row2 + block0)
        limit = begin - lane2 - (block0 - RING * TOK)
        causal = row2 - lane2
        segment_at = segment * PREFIX - lane2
        highest = jnp.full((2 * TOK, HEAD), NEG, jnp.float32)
        for c in range(RING + 2):
            if c <= RING:
                tile = kvbuf[rows(src + c), 0:HEAD]
            else:
                tile = pre[:, 0:HEAD]
            score = lax.dot_general(
                q2[...], tile, contract_last, preferred_element_type=jnp.float32
            )
            for part in range(2):
                at = part * HEAD
                if c < RING:
                    seen = limit <= c * TOK + at
                elif c == RING:
                    seen = (limit <= c * TOK + at) & (causal >= at)
                else:
                    seen = (segment_at <= at) & (segment_at > at - PREFIX)
                piece = jnp.where(seen, score[:, at : at + HEAD], NEG)
                highest = jnp.maximum(highest, piece)
                scores[c, :, at : at + HEAD] = piece
        top = jnp.max(highest, axis=1, keepdims=True)
        total = jnp.zeros((2 * TOK, HEAD), jnp.float32)
        summed = jnp.zeros((2 * TOK, HEAD), jnp.float32)
        for c in range(RING + 2):
            weight = jnp.exp2((scores[c] - top) * LOG2E_SCALE)
            total = total + (weight[:, 0:HEAD] + weight[:, HEAD:PAIR])
            if c <= RING:
                tile = kvbuf[rows(src + c), HEAD:PAIR]
            else:
                tile = pre[:, HEAD:PAIR]
            summed = summed + jnp.dot(
                weight.astype(jnp.bfloat16), tile, preferred_element_type=jnp.float32
            )
        result = (summed / jnp.sum(total, axis=1, keepdims=True)).astype(jnp.bfloat16)
        obuf[d, :, 0:HEAD] = result[0:TOK]
        obuf[d, :, HEAD:PAIR] = result[TOK : 2 * TOK]

        @pl.when(i == 0)
        def _():
            pltpu.make_async_copy(
                obuf.at[0], attended.at[0, :, lanes(z, PAIR)], local.at[2]
            ).start()

        @pl.when(i > 0)
        def _():
            send_o(d).start()

        return carry

    lax.fori_loop(0, RING, one_block, 0)

    for d in range(1, RING):
        send_v(d).wait_send()
        send_k(d).wait_send()
        send_q(d).wait_send()
    for s in range(RING):
        forward(s).wait_send()
    for e in range(1, n_batch):
        send_pool(e).wait_send()
    cache_copy.wait()
    pltpu.make_async_copy(obuf.at[0], attended.at[0, :, lanes(z, PAIR)], local.at[2]).wait()
    for d in range(1, RING):
        send_o(d).wait_send()
        pltpu.make_async_remote_copy(
            src_ref=obuf.at[d],
            dst_ref=attended.at[0, :, lanes(ring(d), PAIR)],
            send_sem=o_send.at[d],
            recv_sem=o_recv.at[d],
            device_id=ring_id(d),
            device_id_type=MESH,
        ).wait_recv()


def per_device(queries, keys, values, seg_ids, lengths, live, page_table, pool):
    n_x = lax.axis_size("blk") // RING
    n_batch = lax.axis_size("batch")
    pool_rows = pool.shape[0]
    half = HEAD // 2
    inverse = np.power(np.float64(ROPE_BASE), -2.0 * np.arange(half) / HEAD)
    freq = jnp.asarray(np.tile(np.concatenate([inverse, inverse])[None], (8, 1)), jnp.float32)

    def body(*refs):
        kernel(n_x, n_batch, pool_rows, *refs)

    bf = jnp.bfloat16
    dma = pltpu.SemaphoreType.DMA
    vmem = pl.BlockSpec(memory_space=pltpu.VMEM)
    smem = pl.BlockSpec(memory_space=pltpu.SMEM)
    anywhere = pl.BlockSpec(memory_space=pl.ANY)
    return pl.pallas_call(
        body,
        out_shape=(
            jax.ShapeDtypeStruct(queries.shape, bf),
            jax.ShapeDtypeStruct(keys.shape, bf),
        ),
        in_specs=[vmem, vmem, anywhere, smem, smem, anywhere, vmem],
        out_specs=(anywhere, anywhere),
        scratch_shapes=[
            pltpu.VMEM((TOK, 2 * KV_HEADS * HEAD), bf),
            pltpu.VMEM((TOK, KV_HEADS * HEAD), bf),
            pltpu.VMEM((RING, TOK, PAIR), bf),
            pltpu.VMEM((2 * RING * TOK, PAIR), bf),
            pltpu.VMEM((n_batch * pool_rows, PAGE, PAIR), bf),
            pltpu.VMEM((pool_rows, PAGE, PAIR), bf),
            pltpu.VMEM((TOK, PAIR), bf),
            pltpu.VMEM((RING + 2, 2 * TOK, TOK), jnp.float32),
            pltpu.VMEM((2 * TOK, HEAD), bf),
            pltpu.VMEM((RING, TOK, PAIR), bf),
            dma((RING,)),
            dma((RING,)),
            dma((RING,)),
            dma((RING,)),
            dma((RING,)),
            dma((RING,)),
            dma((RING,)),
            dma((RING,)),
            dma((n_batch,)),
            dma((n_batch,)),
            dma((RING,)),
            dma((RING,)),
            dma((5,)),
        ],
        compiler_params=pltpu.CompilerParams(
            collective_id=0, has_side_effects=True, vmem_limit_bytes=48 * 1024 * 1024
        ),
    )(queries, keys, values, lengths, page_table, pool, freq)


def solution(mesh):
    in_specs = (
        P("batch", "blk", None),
        P("batch", "blk", None),
        P("batch", "blk", None),
        P("batch", "blk"),
        P("batch", None),
        P("batch", "blk", None),
        P(),
        P("batch", None, None),
    )
    out_specs = (P("batch", "blk", None), P("batch", "blk", None))
    return jax.shard_map(
        per_device, mesh=mesh, in_specs=in_specs, out_specs=out_specs, check_vma=False
    )
```

```python
import math

import jax
import jax.numpy as jnp
import numpy as np
from jax import lax
from jax.experimental import pallas as pl
from jax.experimental.pallas import tpu as pltpu
from jax.sharding import PartitionSpec as P

HEAD = 128
KV_HEADS = 8
RING = 8
TOK = 256
SEGS = 7
PAGES_SEG = 2
PAGE = 16
PREFIX = PAGES_SEG * PAGE
PAIR = 2 * HEAD
ROPE_BASE = 1000000.0
LOG2E_SCALE = math.log2(math.e) / math.sqrt(HEAD)
NEG = -1e30
MESH = pl.DeviceIdType.MESH


def kernel(
    n_x,
    n_batch,
    pool_rows,
    queries,
    keys,
    values,
    lengths,
    page_table,
    pool,
    freq,
    attended,
    cache,
    qraw,
    kraw,
    qrot,
    krot,
    qbuf,
    kvbuf,
    pbuf,
    pown,
    pre,
    scores,
    q2,
    obuf,
    v_send,
    v_recv,
    k_send,
    k_recv,
    q_send,
    q_recv,
    f_send,
    f_recv,
    p_send,
    p_recv,
    o_send,
    o_recv,
    local,
):
    blk = lax.axis_index("blk")
    bat = lax.axis_index("batch")
    z = lax.rem(blk, RING)
    x = lax.div(blk, RING)

    def ring(d):
        return lax.rem(z + d, RING)

    def ring_id(d):
        return (x * RING + ring(d), bat)

    def other(e):
        return lax.rem(bat + e, n_batch)

    def lanes(i, width):
        return pl.ds(pl.multiple_of(i * width, width), width)

    def rows(i):
        return pl.ds(pl.multiple_of(i * TOK, TOK), TOK)

    ahead = (lax.rem(x + 1, n_x) * RING + z, bat)
    behind = (lax.rem(x + n_x - 1, n_x) * RING + z, bat)

    barrier = pltpu.get_barrier_semaphore()
    for d in range(1, RING):
        pl.semaphore_signal(barrier, inc=1, device_id=ring_id(d), device_id_type=MESH)
    for who in (ahead, behind):
        pl.semaphore_signal(barrier, inc=1, device_id=who, device_id_type=MESH)
    for e in range(1, n_batch):
        pl.semaphore_signal(barrier, inc=1, device_id=(blk, other(e)), device_id_type=MESH)
    own_pool_k = pltpu.make_async_copy(pool.at[:, :, lanes(z, HEAD)], pown.at[:, :, 0:HEAD], local.at[0])
    own_pool_v = pltpu.make_async_copy(
        pool.at[:, :, lanes(z + KV_HEADS, HEAD)], pown.at[:, :, HEAD:PAIR], local.at[1]
    )
    own_v = pltpu.make_async_copy(
        values.at[0, :, lanes(z, HEAD)], kvbuf.at[rows(RING + z), HEAD:PAIR], local.at[2]
    )
    load_k = pltpu.make_async_copy(keys.at[0], kraw, local.at[5])
    load_q = pltpu.make_async_copy(queries.at[0], qraw, local.at[6])
    load_k.start()
    own_pool_k.start()
    own_pool_v.start()
    own_v.start()
    load_q.start()
    pl.semaphore_wait(barrier, RING - 1 + 2 + n_batch - 1)

    def send_v(d):
        return pltpu.make_async_remote_copy(
            src_ref=values.at[0, :, lanes(ring(d), HEAD)],
            dst_ref=kvbuf.at[rows(RING + z), HEAD:PAIR],
            send_sem=v_send.at[d],
            recv_sem=v_recv.at[d],
            device_id=ring_id(d),
            device_id_type=MESH,
        )

    def send_k(d):
        return pltpu.make_async_remote_copy(
            src_ref=krot.at[:, lanes(ring(d), HEAD)],
            dst_ref=kvbuf.at[rows(RING + z), 0:HEAD],
            send_sem=k_send.at[d],
            recv_sem=k_recv.at[d],
            device_id=ring_id(d),
            device_id_type=MESH,
        )

    def send_q(d):
        return pltpu.make_async_remote_copy(
            src_ref=qrot.at[:, lanes(ring(d), PAIR)],
            dst_ref=qbuf.at[z],
            send_sem=q_send.at[d],
            recv_sem=q_recv.at[d],
            device_id=ring_id(d),
            device_id_type=MESH,
        )

    def send_pool(e):
        return pltpu.make_async_remote_copy(
            src_ref=pown,
            dst_ref=pbuf.at[pl.ds(bat * pool_rows, pool_rows)],
            send_sem=p_send.at[e],
            recv_sem=p_recv.at[e],
            device_id=(blk, other(e)),
            device_id_type=MESH,
        )

    def forward(s):
        return pltpu.make_async_remote_copy(
            src_ref=kvbuf.at[rows(RING + s)],
            dst_ref=kvbuf.at[rows(s)],
            send_sem=f_send.at[s],
            recv_sem=f_recv.at[s],
            device_id=ahead,
            device_id_type=MESH,
        )

    def send_o(d):
        return pltpu.make_async_remote_copy(
            src_ref=obuf.at[d],
            dst_ref=attended.at[0, :, lanes(z, PAIR)],
            send_sem=o_send.at[d],
            recv_sem=o_recv.at[d],
            device_id=ring_id(RING - d),
            device_id_type=MESH,
        )

    order = (4, 3, 5, 2, 6, 1, 7)
    for d in order:
        send_v(d).start()
    own_pool_k.wait()
    own_pool_v.wait()
    for e in range(1, n_batch):
        send_pool(e).start()
    own_pool = pltpu.make_async_copy(pown, pbuf.at[pl.ds(bat * pool_rows, pool_rows)], local.at[0])
    own_pool.start()

    starts = [jnp.int32(0)]
    for s in range(SEGS - 1):
        starts.append(starts[-1] + lengths[0, s])

    def start_and_segment(token):
        first = jnp.zeros_like(token)
        segment = jnp.zeros_like(token)
        for s in range(1, SEGS):
            inside = token >= starts[s]
            first = jnp.where(inside, starts[s], first)
            segment = jnp.where(inside, s, segment)
        return first, segment

    row = lax.broadcasted_iota(jnp.int32, (TOK, HEAD), 0)
    lane = lax.broadcasted_iota(jnp.int32, (TOK, HEAD), 1)
    token = row + blk * TOK
    first, _ = start_and_segment(token)
    angle = (PREFIX + token - first).astype(jnp.float32) * freq[0:1, :]
    cosine = jnp.cos(angle)
    sine = jnp.sin(angle)
    sine = jnp.where(lane < HEAD // 2, -sine, sine)

    def turn(part):
        part = part.astype(jnp.float32)
        return (part * cosine + pltpu.roll(part, HEAD // 2, 1) * sine).astype(jnp.bfloat16)

    load_k.wait()
    for h in range(KV_HEADS):
        krot[:, h * HEAD : (h + 1) * HEAD] = turn(kraw[:, h * HEAD : (h + 1) * HEAD])
    for d in order:
        send_k(d).start()
    own_k = pltpu.make_async_copy(
        krot.at[:, lanes(z, HEAD)], kvbuf.at[rows(RING + z), 0:HEAD], local.at[1]
    )
    own_k.start()
    cache_copy = pltpu.make_async_copy(krot, cache.at[0], local.at[3])
    cache_copy.start()
    load_q.wait()
    for h in range(2 * KV_HEADS):
        qrot[:, h * HEAD : (h + 1) * HEAD] = turn(qraw[:, h * HEAD : (h + 1) * HEAD])
    for d in order:
        send_q(d).start()
    own_q = pltpu.make_async_copy(qrot.at[:, lanes(z, PAIR)], qbuf.at[z], local.at[4])
    own_q.start()

    own_v.wait()
    own_k.wait()
    forward(z).start()

    def from_ring(sem, width_lo, d):
        src = ring(RING - d)
        view = kvbuf.at[rows(RING + src), width_lo : width_lo + HEAD]
        return pltpu.make_async_remote_copy(
            src_ref=view,
            dst_ref=view,
            send_sem=v_send.at[d],
            recv_sem=sem.at[d],
            device_id=ring_id(RING - d),
            device_id_type=MESH,
        )

    for d in order:
        from_ring(v_recv, HEAD, d).wait_recv()
        from_ring(k_recv, 0, d).wait_recv()
        forward(ring(RING - d)).start()

    own_pool.wait()
    for e in range(1, n_batch):
        src = pl.ds(lax.rem(bat + n_batch - e, n_batch) * pool_rows, pool_rows)
        pltpu.make_async_remote_copy(
            src_ref=pown,
            dst_ref=pbuf.at[src],
            send_sem=p_send.at[e],
            recv_sem=p_recv.at[e],
            device_id=(blk, other(n_batch - e)),
            device_id_type=MESH,
        ).wait_recv()
    for s in range(SEGS):
        for i in range(PAGES_SEG):
            at = s * PREFIX + i * PAGE
            pre[at : at + PAGE, :] = pbuf[page_table[bat, s, i]]
    pre[SEGS * PREFIX :, :] = jnp.zeros((TOK - SEGS * PREFIX, PAIR), jnp.bfloat16)

    for s in range(RING):
        forward(s).wait_recv()

    row2 = lax.rem(lax.broadcasted_iota(jnp.int32, (2 * TOK, HEAD), 0), TOK)
    lane2 = lax.broadcasted_iota(jnp.int32, (2 * TOK, HEAD), 1)
    contract_last = (((1,), (1,)), ((), ()))

    def one_block(i, carry):
        odd = lax.rem(i, 2)
        half = lax.div(i + 1, 2)
        d = RING // 2 + (1 - 2 * odd) * half
        src = ring(RING - d)

        @pl.when(d == 0)
        def _():
            pltpu.make_async_copy(qrot.at[:, lanes(z, PAIR)], qbuf.at[z], local.at[4]).wait()

        @pl.when(d > 0)
        def _():
            pltpu.make_async_remote_copy(
                src_ref=qbuf.at[src],
                dst_ref=qbuf.at[src],
                send_sem=q_send.at[d],
                recv_sem=q_recv.at[d],
                device_id=ring_id(RING - d),
                device_id_type=MESH,
            ).wait_recv()

        q2[0:TOK, :] = qbuf[src, :, 0:HEAD]
        q2[TOK : 2 * TOK, :] = qbuf[src, :, HEAD:PAIR]
        block0 = (x * RING + src) * TOK
        begin, segment = start_and_segment(row2 + block0)
        limit = begin - lane2 - (block0 - RING * TOK)
        causal = row2 - lane2
        segment_at = segment * PREFIX - lane2
        highest = jnp.full((2 * TOK, HEAD), NEG, jnp.float32)
        for c in range(RING + 2):
            if c <= RING:
                tile = kvbuf[rows(src + c), 0:HEAD]
            else:
                tile = pre[:, 0:HEAD]
            score = lax.dot_general(
                q2[...], tile, contract_last, preferred_element_type=jnp.float32
            )
            for part in range(2):
                at = part * HEAD
                if c < RING:
                    seen = limit <= c * TOK + at
                elif c == RING:
                    seen = (limit <= c * TOK + at) & (causal >= at)
                else:
                    seen = (segment_at <= at) & (segment_at > at - PREFIX)
                piece = jnp.where(seen, score[:, at : at + HEAD], NEG)
                highest = jnp.maximum(highest, piece)
                scores[c, :, at : at + HEAD] = piece
        top = jnp.max(highest, axis=1, keepdims=True)
        total = jnp.zeros((2 * TOK, HEAD), jnp.float32)
        summed = jnp.zeros((2 * TOK, HEAD), jnp.float32)
        for c in range(RING + 2):
            weight = jnp.exp2((scores[c] - top) * LOG2E_SCALE)
            total = total + (weight[:, 0:HEAD] + weight[:, HEAD:PAIR])
            if c <= RING:
                tile = kvbuf[rows(src + c), HEAD:PAIR]
            else:
                tile = pre[:, HEAD:PAIR]
            summed = summed + jnp.dot(
                weight.astype(jnp.bfloat16), tile, preferred_element_type=jnp.float32
            )
        result = (summed / jnp.sum(total, axis=1, keepdims=True)).astype(jnp.bfloat16)
        obuf[d, :, 0:HEAD] = result[0:TOK]
        obuf[d, :, HEAD:PAIR] = result[TOK : 2 * TOK]

        @pl.when(d == 0)
        def _():
            pltpu.make_async_copy(
                obuf.at[0], attended.at[0, :, lanes(z, PAIR)], local.at[2]
            ).start()

        @pl.when(d > 0)
        def _():
            send_o(d).start()

        return carry

    lax.fori_loop(0, RING, one_block, 0)

    for d in range(1, RING):
        send_v(d).wait_send()
        send_k(d).wait_send()
        send_q(d).wait_send()
    for s in range(RING):
        forward(s).wait_send()
    for e in range(1, n_batch):
        send_pool(e).wait_send()
    cache_copy.wait()
    pltpu.make_async_copy(obuf.at[0], attended.at[0, :, lanes(z, PAIR)], local.at[2]).wait()
    for d in range(1, RING):
        send_o(d).wait_send()
        pltpu.make_async_remote_copy(
            src_ref=obuf.at[d],
            dst_ref=attended.at[0, :, lanes(ring(d), PAIR)],
            send_sem=o_send.at[d],
            recv_sem=o_recv.at[d],
            device_id=ring_id(d),
            device_id_type=MESH,
        ).wait_recv()


def per_device(queries, keys, values, seg_ids, lengths, live, page_table, pool):
    n_x = lax.axis_size("blk") // RING
    n_batch = lax.axis_size("batch")
    pool_rows = pool.shape[0]
    half = HEAD // 2
    inverse = np.power(np.float64(ROPE_BASE), -2.0 * np.arange(half) / HEAD)
    freq = jnp.asarray(np.tile(np.concatenate([inverse, inverse])[None], (8, 1)), jnp.float32)

    def body(*refs):
        kernel(n_x, n_batch, pool_rows, *refs)

    bf = jnp.bfloat16
    dma = pltpu.SemaphoreType.DMA
    vmem = pl.BlockSpec(memory_space=pltpu.VMEM)
    smem = pl.BlockSpec(memory_space=pltpu.SMEM)
    anywhere = pl.BlockSpec(memory_space=pl.ANY)
    return pl.pallas_call(
        body,
        out_shape=(
            jax.ShapeDtypeStruct(queries.shape, bf),
            jax.ShapeDtypeStruct(keys.shape, bf),
        ),
        in_specs=[anywhere, anywhere, anywhere, smem, smem, anywhere, vmem],
        out_specs=(anywhere, anywhere),
        scratch_shapes=[
            pltpu.VMEM((TOK, 2 * KV_HEADS * HEAD), bf),
            pltpu.VMEM((TOK, KV_HEADS * HEAD), bf),
            pltpu.VMEM((TOK, 2 * KV_HEADS * HEAD), bf),
            pltpu.VMEM((TOK, KV_HEADS * HEAD), bf),
            pltpu.VMEM((RING, TOK, PAIR), bf),
            pltpu.VMEM((2 * RING * TOK, PAIR), bf),
            pltpu.VMEM((n_batch * pool_rows, PAGE, PAIR), bf),
            pltpu.VMEM((pool_rows, PAGE, PAIR), bf),
            pltpu.VMEM((TOK, PAIR), bf),
            pltpu.VMEM((RING + 2, 2 * TOK, TOK), jnp.float32),
            pltpu.VMEM((2 * TOK, HEAD), bf),
            pltpu.VMEM((RING, TOK, PAIR), bf),
            dma((RING,)),
            dma((RING,)),
            dma((RING,)),
            dma((RING,)),
            dma((RING,)),
            dma((RING,)),
            dma((RING,)),
            dma((RING,)),
            dma((n_batch,)),
            dma((n_batch,)),
            dma((RING,)),
            dma((RING,)),
            dma((7,)),
        ],
        compiler_params=pltpu.CompilerParams(
            collective_id=0, has_side_effects=True, vmem_limit_bytes=67043328
        ),
    )(queries, keys, values, lengths, page_table, pool, freq)


def solution(mesh):
    in_specs = (
        P("batch", "blk", None),
        P("batch", "blk", None),
        P("batch", "blk", None),
        P("batch", "blk"),
        P("batch", None),
        P("batch", "blk", None),
        P(),
        P("batch", None, None),
    )
    out_specs = (P("batch", "blk", None), P("batch", "blk", None))
    return jax.shard_map(
        per_device, mesh=mesh, in_specs=in_specs, out_specs=out_specs, check_vma=False
    )
```

```python
import math

import jax
import jax.numpy as jnp
import numpy as np
from jax import lax
from jax.experimental import pallas as pl
from jax.experimental.pallas import tpu as pltpu
from jax.sharding import PartitionSpec as P

HEAD = 128
KV_HEADS = 8
RING = 8
TOK = 256
SEGS = 7
PAGES_SEG = 2
PAGE = 16
PREFIX = PAGES_SEG * PAGE
PAIR = 2 * HEAD
ROPE_BASE = 1000000.0
LOG2E_SCALE = math.log2(math.e) / math.sqrt(HEAD)
NEG = -1e30
MESH = pl.DeviceIdType.MESH


def kernel(
    n_x,
    n_batch,
    pool_rows,
    queries,
    keys,
    values,
    lengths,
    page_table,
    pool,
    freq,
    attended,
    cache,
    qraw,
    kraw,
    qrot,
    krot,
    vown,
    qbuf,
    kbuf,
    vbuf,
    pbuf,
    pown,
    pre,
    scores,
    q2,
    obuf,
    v_send,
    v_recv,
    k_send,
    k_recv,
    q_send,
    q_recv,
    fv_send,
    fv_recv,
    fk_send,
    fk_recv,
    p_send,
    p_recv,
    o_send,
    o_recv,
    local,
    v_load,
):
    blk = lax.axis_index("blk")
    bat = lax.axis_index("batch")
    z = lax.rem(blk, RING)
    x = lax.div(blk, RING)

    def ring(d):
        return lax.rem(z + d, RING)

    def ring_id(d):
        return (x * RING + ring(d), bat)

    def other(e):
        return lax.rem(bat + e, n_batch)

    def lanes(i, width):
        return pl.ds(pl.multiple_of(i * width, width), width)

    def rows(i):
        return pl.ds(pl.multiple_of(i * TOK, TOK), TOK)

    ahead = (lax.rem(x + 1, n_x) * RING + z, bat)
    behind = (lax.rem(x + n_x - 1, n_x) * RING + z, bat)

    barrier = pltpu.get_barrier_semaphore()
    for d in range(1, RING):
        pl.semaphore_signal(barrier, inc=1, device_id=ring_id(d), device_id_type=MESH)
    for who in (ahead, behind):
        pl.semaphore_signal(barrier, inc=1, device_id=who, device_id_type=MESH)
    for e in range(1, n_batch):
        pl.semaphore_signal(barrier, inc=1, device_id=(blk, other(e)), device_id_type=MESH)
    own_pool_k = pltpu.make_async_copy(pool.at[:, :, lanes(z, HEAD)], pown.at[:, :, 0:HEAD], local.at[0])
    own_pool_v = pltpu.make_async_copy(
        pool.at[:, :, lanes(z + KV_HEADS, HEAD)], pown.at[:, :, HEAD:PAIR], local.at[1]
    )
    load_v = [
        pltpu.make_async_copy(values.at[0, :, h * HEAD : (h + 1) * HEAD], vown.at[h], v_load.at[h])
        for h in range(KV_HEADS)
    ]
    load_k = pltpu.make_async_copy(keys.at[0], kraw, local.at[5])
    load_q = pltpu.make_async_copy(queries.at[0], qraw, local.at[6])
    for copy in load_v:
        copy.start()
    load_k.start()
    own_pool_k.start()
    own_pool_v.start()
    load_q.start()
    pl.semaphore_wait(barrier, RING - 1 + 2 + n_batch - 1)

    def send_v(d):
        return pltpu.make_async_remote_copy(
            src_ref=vown.at[ring(d)],
            dst_ref=vbuf.at[rows(RING + z)],
            send_sem=v_send.at[d],
            recv_sem=v_recv.at[d],
            device_id=ring_id(d),
            device_id_type=MESH,
        )

    def send_k(d):
        return pltpu.make_async_remote_copy(
            src_ref=krot.at[ring(d)],
            dst_ref=kbuf.at[rows(RING + z)],
            send_sem=k_send.at[d],
            recv_sem=k_recv.at[d],
            device_id=ring_id(d),
            device_id_type=MESH,
        )

    def send_q(d):
        return pltpu.make_async_remote_copy(
            src_ref=qrot.at[ring(d)],
            dst_ref=qbuf.at[z],
            send_sem=q_send.at[d],
            recv_sem=q_recv.at[d],
            device_id=ring_id(d),
            device_id_type=MESH,
        )

    def send_pool(e):
        return pltpu.make_async_remote_copy(
            src_ref=pown,
            dst_ref=pbuf.at[pl.ds(bat * pool_rows, pool_rows)],
            send_sem=p_send.at[e],
            recv_sem=p_recv.at[e],
            device_id=(blk, other(e)),
            device_id_type=MESH,
        )

    def forward(buf, sends, recvs, s, src=None):
        return pltpu.make_async_remote_copy(
            src_ref=buf.at[rows(RING + s)] if src is None else src,
            dst_ref=buf.at[rows(s)],
            send_sem=sends.at[s],
            recv_sem=recvs.at[s],
            device_id=ahead,
            device_id_type=MESH,
        )

    def forward_v(s, src=None):
        return forward(vbuf, fv_send, fv_recv, s, src)

    def forward_k(s, src=None):
        return forward(kbuf, fk_send, fk_recv, s, src)

    def send_o(d):
        return pltpu.make_async_remote_copy(
            src_ref=obuf.at[d],
            dst_ref=attended.at[z],
            send_sem=o_send.at[d],
            recv_sem=o_recv.at[d],
            device_id=ring_id(RING - d),
            device_id_type=MESH,
        )

    order = (4, 3, 5, 2, 6, 1, 7)
    for copy in load_v:
        copy.wait()
    for d in order:
        send_v(d).start()
    own_v = pltpu.make_async_copy(vown.at[z], vbuf.at[rows(RING + z)], local.at[2])
    own_v.start()
    forward_v(z, vown.at[z]).start()
    own_pool_k.wait()
    own_pool_v.wait()
    for e in range(1, n_batch):
        send_pool(e).start()
    own_pool = pltpu.make_async_copy(pown, pbuf.at[pl.ds(bat * pool_rows, pool_rows)], local.at[0])
    own_pool.start()

    starts = [jnp.int32(0)]
    for s in range(SEGS - 1):
        starts.append(starts[-1] + lengths[0, s])

    def start_and_segment(token):
        first = jnp.zeros_like(token)
        segment = jnp.zeros_like(token)
        for s in range(1, SEGS):
            inside = token >= starts[s]
            first = jnp.where(inside, starts[s], first)
            segment = jnp.where(inside, s, segment)
        return first, segment

    row = lax.broadcasted_iota(jnp.int32, (TOK, HEAD), 0)
    lane = lax.broadcasted_iota(jnp.int32, (TOK, HEAD), 1)
    token = row + blk * TOK
    first, _ = start_and_segment(token)
    angle = (PREFIX + token - first).astype(jnp.float32) * freq[0:1, :]
    cosine = jnp.cos(angle)
    sine = jnp.sin(angle)
    sine = jnp.where(lane < HEAD // 2, -sine, sine)

    def turn(part):
        part = part.astype(jnp.float32)
        return (part * cosine + pltpu.roll(part, HEAD // 2, 1) * sine).astype(jnp.bfloat16)

    load_k.wait()
    for h in range(KV_HEADS):
        krot[h] = turn(kraw[:, h * HEAD : (h + 1) * HEAD])
    for d in order:
        send_k(d).start()
    own_k = pltpu.make_async_copy(krot.at[z], kbuf.at[rows(RING + z)], local.at[1])
    own_k.start()
    forward_k(z, krot.at[z]).start()
    cache_copy = pltpu.make_async_copy(krot, cache, local.at[3])
    cache_copy.start()
    load_q.wait()
    for h in range(2 * KV_HEADS):
        at = (h % 2) * HEAD
        qrot[h // 2, :, at : at + HEAD] = turn(qraw[:, h * HEAD : (h + 1) * HEAD])
    for d in order:
        send_q(d).start()
    own_q = pltpu.make_async_copy(qrot.at[z], qbuf.at[z], local.at[4])
    own_q.start()

    def from_ring(buf, recvs, d):
        view = buf.at[rows(RING + ring(RING - d))]
        return pltpu.make_async_remote_copy(
            src_ref=view,
            dst_ref=view,
            send_sem=v_send.at[d],
            recv_sem=recvs.at[d],
            device_id=ring_id(RING - d),
            device_id_type=MESH,
        )

    for d in order:
        from_ring(vbuf, v_recv, d).wait_recv()
        forward_v(ring(RING - d)).start()
    for d in order:
        from_ring(kbuf, k_recv, d).wait_recv()
        forward_k(ring(RING - d)).start()
    own_v.wait()
    own_k.wait()

    own_pool.wait()
    for e in range(1, n_batch):
        src = pl.ds(lax.rem(bat + n_batch - e, n_batch) * pool_rows, pool_rows)
        pltpu.make_async_remote_copy(
            src_ref=pown,
            dst_ref=pbuf.at[src],
            send_sem=p_send.at[e],
            recv_sem=p_recv.at[e],
            device_id=(blk, other(n_batch - e)),
            device_id_type=MESH,
        ).wait_recv()
    for s in range(SEGS):
        for i in range(PAGES_SEG):
            at = s * PREFIX + i * PAGE
            pre[at : at + PAGE, :] = pbuf[page_table[s, i, bat]]
    pre[SEGS * PREFIX :, :] = jnp.zeros((TOK - SEGS * PREFIX, PAIR), jnp.bfloat16)

    for s in range(RING):
        forward_v(s).wait_recv()
        forward_k(s).wait_recv()

    row2 = lax.rem(lax.broadcasted_iota(jnp.int32, (2 * TOK, HEAD), 0), TOK)
    lane2 = lax.broadcasted_iota(jnp.int32, (2 * TOK, HEAD), 1)
    contract_last = (((1,), (1,)), ((), ()))

    def one_block(i, carry):
        odd = lax.rem(i, 2)
        half = lax.div(i + 1, 2)
        d = RING // 2 + (1 - 2 * odd) * half
        src = ring(RING - d)

        @pl.when(d == 0)
        def _():
            pltpu.make_async_copy(qrot.at[z], qbuf.at[z], local.at[4]).wait()

        @pl.when(d > 0)
        def _():
            pltpu.make_async_remote_copy(
                src_ref=qbuf.at[src],
                dst_ref=qbuf.at[src],
                send_sem=q_send.at[d],
                recv_sem=q_recv.at[d],
                device_id=ring_id(RING - d),
                device_id_type=MESH,
            ).wait_recv()

        q2[0:TOK, :] = qbuf[src, :, 0:HEAD]
        q2[TOK : 2 * TOK, :] = qbuf[src, :, HEAD:PAIR]
        block0 = (x * RING + src) * TOK
        begin, segment = start_and_segment(row2 + block0)
        limit = begin - lane2 - (block0 - RING * TOK)
        causal = row2 - lane2
        segment_at = segment * PREFIX - lane2
        highest = jnp.full((2 * TOK, HEAD), NEG, jnp.float32)
        for c in range(RING + 2):
            if c <= RING:
                tile = kbuf[rows(src + c), :]
            else:
                tile = pre[:, 0:HEAD]
            score = lax.dot_general(
                q2[...], tile, contract_last, preferred_element_type=jnp.float32
            )
            for part in range(2):
                at = part * HEAD
                if c < RING:
                    seen = limit <= c * TOK + at
                elif c == RING:
                    seen = (limit <= c * TOK + at) & (causal >= at)
                else:
                    seen = (segment_at <= at) & (segment_at > at - PREFIX)
                piece = jnp.where(seen, score[:, at : at + HEAD], NEG)
                highest = jnp.maximum(highest, piece)
                scores[c, :, at : at + HEAD] = piece
        top = jnp.max(highest, axis=1, keepdims=True)
        total = jnp.zeros((2 * TOK, HEAD), jnp.float32)
        summed = jnp.zeros((2 * TOK, HEAD), jnp.float32)
        for c in range(RING + 2):
            weight = jnp.exp2((scores[c] - top) * LOG2E_SCALE)
            total = total + (weight[:, 0:HEAD] + weight[:, HEAD:PAIR])
            if c <= RING:
                tile = vbuf[rows(src + c), :]
            else:
                tile = pre[:, HEAD:PAIR]
            summed = summed + jnp.dot(
                weight.astype(jnp.bfloat16), tile, preferred_element_type=jnp.float32
            )
        result = (summed / jnp.sum(total, axis=1, keepdims=True)).astype(jnp.bfloat16)
        obuf[d, :, 0:HEAD] = result[0:TOK]
        obuf[d, :, HEAD:PAIR] = result[TOK : 2 * TOK]

        @pl.when(d == 0)
        def _():
            pltpu.make_async_copy(
                obuf.at[0], attended.at[z], local.at[2]
            ).start()

        @pl.when(d > 0)
        def _():
            send_o(d).start()

        return carry

    lax.fori_loop(0, RING, one_block, 0)

    for d in range(1, RING):
        send_v(d).wait_send()
        send_k(d).wait_send()
        send_q(d).wait_send()
    for s in range(RING):
        forward_v(s).wait_send()
        forward_k(s).wait_send()
    for e in range(1, n_batch):
        send_pool(e).wait_send()
    cache_copy.wait()
    pltpu.make_async_copy(obuf.at[0], attended.at[z], local.at[2]).wait()
    for d in range(1, RING):
        send_o(d).wait_send()
        pltpu.make_async_remote_copy(
            src_ref=obuf.at[d],
            dst_ref=attended.at[ring(d)],
            send_sem=o_send.at[d],
            recv_sem=o_recv.at[d],
            device_id=ring_id(d),
            device_id_type=MESH,
        ).wait_recv()


def finish(heads, rotated, attended, cache, h_buf, r_buf, h_in, r_in, h_out, r_out):
    loads = []
    for s in range(KV_HEADS):
        loads.append(pltpu.make_async_copy(heads.at[s], h_buf.at[s], h_in.at[s]))
        loads.append(pltpu.make_async_copy(rotated.at[s], r_buf.at[s], r_in.at[s]))
    for copy in loads:
        copy.start()
    stores = []
    for s in range(KV_HEADS):
        stores.append(
            pltpu.make_async_copy(
                h_buf.at[s], attended.at[0, :, s * PAIR : (s + 1) * PAIR], h_out.at[s]
            )
        )
        stores.append(
            pltpu.make_async_copy(
                r_buf.at[s], cache.at[0, :, s * HEAD : (s + 1) * HEAD], r_out.at[s]
            )
        )
    for load, store in zip(loads, stores):
        load.wait()
        store.start()
    for copy in stores:
        copy.wait()


def per_device(queries, keys, values, seg_ids, lengths, live, page_table, pool):
    n_x = lax.axis_size("blk") // RING
    n_batch = lax.axis_size("batch")
    pool_rows = pool.shape[0]
    half = HEAD // 2
    inverse = np.power(np.float64(ROPE_BASE), -2.0 * np.arange(half) / HEAD)
    freq = jnp.asarray(np.tile(np.concatenate([inverse, inverse])[None], (8, 1)), jnp.float32)

    def body(*refs):
        kernel(n_x, n_batch, pool_rows, *refs)

    bf = jnp.bfloat16
    dma = pltpu.SemaphoreType.DMA
    vmem = pl.BlockSpec(memory_space=pltpu.VMEM)
    smem = pl.BlockSpec(memory_space=pltpu.SMEM)
    anywhere = pl.BlockSpec(memory_space=pl.ANY)
    heads, rotated = pl.pallas_call(
        body,
        out_shape=(
            jax.ShapeDtypeStruct((KV_HEADS, TOK, PAIR), bf),
            jax.ShapeDtypeStruct((KV_HEADS, TOK, HEAD), bf),
        ),
        in_specs=[anywhere, anywhere, anywhere, smem, smem, anywhere, vmem],
        out_specs=(anywhere, anywhere),
        scratch_shapes=[
            pltpu.VMEM((TOK, 2 * KV_HEADS * HEAD), bf),
            pltpu.VMEM((TOK, KV_HEADS * HEAD), bf),
            pltpu.VMEM((KV_HEADS, TOK, PAIR), bf),
            pltpu.VMEM((KV_HEADS, TOK, HEAD), bf),
            pltpu.VMEM((KV_HEADS, TOK, HEAD), bf),
            pltpu.VMEM((RING, TOK, PAIR), bf),
            pltpu.VMEM((2 * RING * TOK, HEAD), bf),
            pltpu.VMEM((2 * RING * TOK, HEAD), bf),
            pltpu.VMEM((n_batch * pool_rows, PAGE, PAIR), bf),
            pltpu.VMEM((pool_rows, PAGE, PAIR), bf),
            pltpu.VMEM((TOK, PAIR), bf),
            pltpu.VMEM((RING + 2, 2 * TOK, TOK), jnp.float32),
            pltpu.VMEM((2 * TOK, HEAD), bf),
            pltpu.VMEM((RING, TOK, PAIR), bf),
            dma((RING,)),
            dma((RING,)),
            dma((RING,)),
            dma((RING,)),
            dma((RING,)),
            dma((RING,)),
            dma((RING,)),
            dma((RING,)),
            dma((RING,)),
            dma((RING,)),
            dma((n_batch,)),
            dma((n_batch,)),
            dma((RING,)),
            dma((RING,)),
            dma((7,)),
            dma((KV_HEADS,)),
        ],
        compiler_params=pltpu.CompilerParams(
            collective_id=0, has_side_effects=True, vmem_limit_bytes=67043328
        ),
    )(queries, keys, values, lengths, jnp.transpose(page_table, (1, 2, 0)), pool, freq)
    return pl.pallas_call(
        finish,
        out_shape=(
            jax.ShapeDtypeStruct(queries.shape, bf),
            jax.ShapeDtypeStruct(keys.shape, bf),
        ),
        in_specs=[anywhere, anywhere],
        out_specs=(anywhere, anywhere),
        scratch_shapes=[
            pltpu.VMEM((KV_HEADS, TOK, PAIR), bf),
            pltpu.VMEM((KV_HEADS, TOK, HEAD), bf),
            dma((KV_HEADS,)),
            dma((KV_HEADS,)),
            dma((KV_HEADS,)),
            dma((KV_HEADS,)),
        ],
        compiler_params=pltpu.CompilerParams(vmem_limit_bytes=67043328),
    )(heads, rotated)


def solution(mesh):
    in_specs = (
        P("batch", "blk", None),
        P("batch", "blk", None),
        P("batch", "blk", None),
        P("batch", "blk"),
        P("batch", None),
        P("batch", "blk", None),
        P(),
        P("batch", None, None),
    )
    out_specs = (P("batch", "blk", None), P("batch", "blk", None))
    return jax.shard_map(
        per_device, mesh=mesh, in_specs=in_specs, out_specs=out_specs, check_vma=False
    )
```

```python
import math

import jax
import jax.numpy as jnp
import numpy as np
from jax import lax
from jax.experimental import pallas as pl
from jax.experimental.pallas import tpu as pltpu
from jax.sharding import PartitionSpec as P

HEAD = 128
KV_HEADS = 8
RING = 8
TOK = 256
SEGS = 7
PAGES_SEG = 2
PAGE = 16
PREFIX = PAGES_SEG * PAGE
PAIR = 2 * HEAD
ROPE_BASE = 1000000.0
LOG2E_SCALE = math.log2(math.e) / math.sqrt(HEAD)
NEG = -1e30
MESH = pl.DeviceIdType.MESH


def kernel(
    n_x,
    n_batch,
    pool_rows,
    queries,
    keys,
    values,
    lengths,
    page_table,
    pool,
    freq,
    attended,
    cache,
    qraw,
    kraw,
    qrot,
    krot,
    vown,
    qbuf,
    kbuf,
    vbuf,
    pbuf,
    pown,
    pre,
    scores,
    q2,
    obuf,
    v_send,
    v_recv,
    k_send,
    k_recv,
    q_send,
    q_recv,
    fv_send,
    fv_recv,
    fk_send,
    fk_recv,
    p_send,
    p_recv,
    o_send,
    o_recv,
    local,
    v_load,
):
    blk = lax.axis_index("blk")
    bat = lax.axis_index("batch")
    z = lax.rem(blk, RING)
    x = lax.div(blk, RING)

    def ring(d):
        return lax.rem(z + d, RING)

    def ring_id(d):
        return (x * RING + ring(d), bat)

    def other(e):
        return lax.rem(bat + e, n_batch)

    def lanes(i, width):
        return pl.ds(pl.multiple_of(i * width, width), width)

    def rows(i):
        return pl.ds(pl.multiple_of(i * TOK, TOK), TOK)

    ahead = (lax.rem(x + 1, n_x) * RING + z, bat)
    behind = (lax.rem(x + n_x - 1, n_x) * RING + z, bat)

    barrier = pltpu.get_barrier_semaphore()
    for d in range(1, RING):
        pl.semaphore_signal(barrier, inc=1, device_id=ring_id(d), device_id_type=MESH)
    for who in (ahead, behind):
        pl.semaphore_signal(barrier, inc=1, device_id=who, device_id_type=MESH)
    for e in range(1, n_batch):
        pl.semaphore_signal(barrier, inc=1, device_id=(blk, other(e)), device_id_type=MESH)
    own_pool_k = pltpu.make_async_copy(pool.at[:, :, lanes(z, HEAD)], pown.at[:, :, 0:HEAD], local.at[0])
    own_pool_v = pltpu.make_async_copy(
        pool.at[:, :, lanes(z + KV_HEADS, HEAD)], pown.at[:, :, HEAD:PAIR], local.at[1]
    )
    def load_v(d):
        return pltpu.make_async_copy(
            values.at[0, :, lanes(ring(d), HEAD)], vown.at[ring(d)], v_load.at[d]
        )

    order = (4, 3, 5, 2, 6, 1, 7)
    load_k = pltpu.make_async_copy(keys.at[0], kraw, local.at[5])
    load_q = pltpu.make_async_copy(queries.at[0], qraw, local.at[6])
    for d in order + (0,):
        load_v(d).start()
    load_k.start()
    own_pool_k.start()
    own_pool_v.start()
    load_q.start()
    pl.semaphore_wait(barrier, RING - 1 + 2 + n_batch - 1)

    def send_v(d):
        return pltpu.make_async_remote_copy(
            src_ref=vown.at[ring(d)],
            dst_ref=vbuf.at[rows(RING + z)],
            send_sem=v_send.at[d],
            recv_sem=v_recv.at[d],
            device_id=ring_id(d),
            device_id_type=MESH,
        )

    def send_k(d):
        return pltpu.make_async_remote_copy(
            src_ref=krot.at[ring(d)],
            dst_ref=kbuf.at[rows(RING + z)],
            send_sem=k_send.at[d],
            recv_sem=k_recv.at[d],
            device_id=ring_id(d),
            device_id_type=MESH,
        )

    def send_q(d):
        return pltpu.make_async_remote_copy(
            src_ref=qrot.at[ring(d)],
            dst_ref=qbuf.at[z],
            send_sem=q_send.at[d],
            recv_sem=q_recv.at[d],
            device_id=ring_id(d),
            device_id_type=MESH,
        )

    def send_pool(e):
        return pltpu.make_async_remote_copy(
            src_ref=pown,
            dst_ref=pbuf.at[pl.ds(bat * pool_rows, pool_rows)],
            send_sem=p_send.at[e],
            recv_sem=p_recv.at[e],
            device_id=(blk, other(e)),
            device_id_type=MESH,
        )

    def forward(buf, sends, recvs, s, src=None):
        return pltpu.make_async_remote_copy(
            src_ref=buf.at[rows(RING + s)] if src is None else src,
            dst_ref=buf.at[rows(s)],
            send_sem=sends.at[s],
            recv_sem=recvs.at[s],
            device_id=ahead,
            device_id_type=MESH,
        )

    def forward_v(s, src=None):
        return forward(vbuf, fv_send, fv_recv, s, src)

    def forward_k(s, src=None):
        return forward(kbuf, fk_send, fk_recv, s, src)

    def send_o(d):
        return pltpu.make_async_remote_copy(
            src_ref=obuf.at[d],
            dst_ref=attended.at[z],
            send_sem=o_send.at[d],
            recv_sem=o_recv.at[d],
            device_id=ring_id(RING - d),
            device_id_type=MESH,
        )

    for d in order:
        load_v(d).wait()
        send_v(d).start()
    load_v(0).wait()
    own_v = pltpu.make_async_copy(vown.at[z], vbuf.at[rows(RING + z)], local.at[2])
    own_v.start()
    forward_v(z, vown.at[z]).start()
    own_pool_k.wait()
    own_pool_v.wait()
    for e in range(1, n_batch):
        send_pool(e).start()
    own_pool = pltpu.make_async_copy(pown, pbuf.at[pl.ds(bat * pool_rows, pool_rows)], local.at[0])
    own_pool.start()

    starts = [jnp.int32(0)]
    for s in range(SEGS - 1):
        starts.append(starts[-1] + lengths[0, s])

    def start_and_segment(token):
        first = jnp.zeros_like(token)
        segment = jnp.zeros_like(token)
        for s in range(1, SEGS):
            inside = token >= starts[s]
            first = jnp.where(inside, starts[s], first)
            segment = jnp.where(inside, s, segment)
        return first, segment

    row = lax.broadcasted_iota(jnp.int32, (TOK, HEAD), 0)
    lane = lax.broadcasted_iota(jnp.int32, (TOK, HEAD), 1)
    token = row + blk * TOK
    first, _ = start_and_segment(token)
    angle = (PREFIX + token - first).astype(jnp.float32) * freq[0:1, :]
    cosine = jnp.cos(angle)
    sine = jnp.sin(angle)
    sine = jnp.where(lane < HEAD // 2, -sine, sine)

    def turn(part):
        part = part.astype(jnp.float32)
        return (part * cosine + pltpu.roll(part, HEAD // 2, 1) * sine).astype(jnp.bfloat16)

    load_k.wait()
    for h in range(KV_HEADS):
        krot[h] = turn(kraw[:, h * HEAD : (h + 1) * HEAD])
    for d in order:
        send_k(d).start()
    own_k = pltpu.make_async_copy(krot.at[z], kbuf.at[rows(RING + z)], local.at[1])
    own_k.start()
    forward_k(z, krot.at[z]).start()
    cache_copy = pltpu.make_async_copy(krot, cache, local.at[3])
    cache_copy.start()
    load_q.wait()
    for h in range(2 * KV_HEADS):
        at = (h % 2) * HEAD
        qrot[h // 2, :, at : at + HEAD] = turn(qraw[:, h * HEAD : (h + 1) * HEAD])
    for d in order:
        send_q(d).start()
    own_q = pltpu.make_async_copy(qrot.at[z], qbuf.at[z], local.at[4])
    own_q.start()

    def from_ring(buf, recvs, d):
        view = buf.at[rows(RING + ring(RING - d))]
        return pltpu.make_async_remote_copy(
            src_ref=view,
            dst_ref=view,
            send_sem=v_send.at[d],
            recv_sem=recvs.at[d],
            device_id=ring_id(RING - d),
            device_id_type=MESH,
        )

    for d in order:
        from_ring(vbuf, v_recv, d).wait_recv()
        forward_v(ring(RING - d)).start()
    for d in order:
        from_ring(kbuf, k_recv, d).wait_recv()
        forward_k(ring(RING - d)).start()
    own_v.wait()
    own_k.wait()

    own_pool.wait()
    for e in range(1, n_batch):
        src = pl.ds(lax.rem(bat + n_batch - e, n_batch) * pool_rows, pool_rows)
        pltpu.make_async_remote_copy(
            src_ref=pown,
            dst_ref=pbuf.at[src],
            send_sem=p_send.at[e],
            recv_sem=p_recv.at[e],
            device_id=(blk, other(n_batch - e)),
            device_id_type=MESH,
        ).wait_recv()
    for s in range(SEGS):
        for i in range(PAGES_SEG):
            at = s * PREFIX + i * PAGE
            pre[at : at + PAGE, :] = pbuf[page_table[s, i, bat]]
    pre[SEGS * PREFIX :, :] = jnp.zeros((TOK - SEGS * PREFIX, PAIR), jnp.bfloat16)

    for s in range(RING):
        forward_v(s).wait_recv()
        forward_k(s).wait_recv()

    contract_last = (((1,), (1,)), ((), ()))

    def one_block(i, carry):
        odd = lax.rem(i, 2)
        half = lax.div(i + 1, 2)
        d = RING // 2 + (1 - 2 * odd) * half
        src = ring(RING - d)

        @pl.when(d == 0)
        def _():
            pltpu.make_async_copy(qrot.at[z], qbuf.at[z], local.at[4]).wait()

        @pl.when(d > 0)
        def _():
            pltpu.make_async_remote_copy(
                src_ref=qbuf.at[src],
                dst_ref=qbuf.at[src],
                send_sem=q_send.at[d],
                recv_sem=q_recv.at[d],
                device_id=ring_id(RING - d),
                device_id_type=MESH,
            ).wait_recv()

        q2[0:TOK, :] = qbuf[src, :, 0:HEAD]
        q2[TOK : 2 * TOK, :] = qbuf[src, :, HEAD:PAIR]
        block0 = (x * RING + src) * TOK
        begin, segment = start_and_segment(row + block0)
        limit = begin - lane - (block0 - RING * TOK)
        causal = row - lane
        segment_at = segment * PREFIX - lane
        highest = [jnp.full((TOK, HEAD), NEG, jnp.float32)] * 2
        for c in range(RING + 2):
            if c <= RING:
                tile = kbuf[rows(src + c), :]
            else:
                tile = pre[:, 0:HEAD]
            score = lax.dot_general(
                q2[...], tile, contract_last, preferred_element_type=jnp.float32
            )
            for part in range(2):
                at = part * HEAD
                if c < RING:
                    seen = limit <= c * TOK + at
                elif c == RING:
                    seen = (limit <= c * TOK + at) & (causal >= at)
                else:
                    seen = (segment_at <= at) & (segment_at > at - PREFIX)
                for g in range(2):
                    own = slice(g * TOK, (g + 1) * TOK)
                    piece = jnp.where(seen, score[own, at : at + HEAD], NEG)
                    highest[g] = jnp.maximum(highest[g], piece)
                    scores[c, own, at : at + HEAD] = piece
        top = jnp.concatenate([jnp.max(part, axis=1, keepdims=True) for part in highest], axis=0)
        total = jnp.zeros((2 * TOK, HEAD), jnp.float32)
        summed = jnp.zeros((2 * TOK, HEAD), jnp.float32)
        for c in range(RING + 2):
            weight = jnp.exp2((scores[c] - top) * LOG2E_SCALE)
            total = total + (weight[:, 0:HEAD] + weight[:, HEAD:PAIR])
            if c <= RING:
                tile = vbuf[rows(src + c), :]
            else:
                tile = pre[:, HEAD:PAIR]
            summed = summed + jnp.dot(
                weight.astype(jnp.bfloat16), tile, preferred_element_type=jnp.float32
            )
        result = (summed / jnp.sum(total, axis=1, keepdims=True)).astype(jnp.bfloat16)
        obuf[d, :, 0:HEAD] = result[0:TOK]
        obuf[d, :, HEAD:PAIR] = result[TOK : 2 * TOK]

        @pl.when(d == 0)
        def _():
            pltpu.make_async_copy(
                obuf.at[0], attended.at[z], local.at[2]
            ).start()

        @pl.when(d > 0)
        def _():
            send_o(d).start()

        return carry

    lax.fori_loop(0, RING, one_block, 0)

    for d in range(1, RING):
        send_v(d).wait_send()
        send_k(d).wait_send()
        send_q(d).wait_send()
    for s in range(RING):
        forward_v(s).wait_send()
        forward_k(s).wait_send()
    for e in range(1, n_batch):
        send_pool(e).wait_send()
    cache_copy.wait()
    pltpu.make_async_copy(obuf.at[0], attended.at[z], local.at[2]).wait()
    for d in range(1, RING):
        send_o(d).wait_send()
        pltpu.make_async_remote_copy(
            src_ref=obuf.at[d],
            dst_ref=attended.at[ring(d)],
            send_sem=o_send.at[d],
            recv_sem=o_recv.at[d],
            device_id=ring_id(d),
            device_id_type=MESH,
        ).wait_recv()


def finish(heads, rotated, attended, cache, h_buf, r_buf, h_in, r_in, h_out, r_out):
    loads = []
    for s in range(KV_HEADS):
        loads.append(pltpu.make_async_copy(heads.at[s], h_buf.at[s], h_in.at[s]))
        loads.append(pltpu.make_async_copy(rotated.at[s], r_buf.at[s], r_in.at[s]))
    for copy in loads:
        copy.start()
    stores = []
    for s in range(KV_HEADS):
        stores.append(
            pltpu.make_async_copy(
                h_buf.at[s], attended.at[0, :, s * PAIR : (s + 1) * PAIR], h_out.at[s]
            )
        )
        stores.append(
            pltpu.make_async_copy(
                r_buf.at[s], cache.at[0, :, s * HEAD : (s + 1) * HEAD], r_out.at[s]
            )
        )
    for load, store in zip(loads, stores):
        load.wait()
        store.start()
    for copy in stores:
        copy.wait()


def per_device(queries, keys, values, seg_ids, lengths, live, page_table, pool):
    n_x = lax.axis_size("blk") // RING
    n_batch = lax.axis_size("batch")
    pool_rows = pool.shape[0]
    half = HEAD // 2
    inverse = np.power(np.float64(ROPE_BASE), -2.0 * np.arange(half) / HEAD)
    freq = jnp.asarray(np.tile(np.concatenate([inverse, inverse])[None], (8, 1)), jnp.float32)

    def body(*refs):
        kernel(n_x, n_batch, pool_rows, *refs)

    bf = jnp.bfloat16
    dma = pltpu.SemaphoreType.DMA
    vmem = pl.BlockSpec(memory_space=pltpu.VMEM)
    smem = pl.BlockSpec(memory_space=pltpu.SMEM)
    anywhere = pl.BlockSpec(memory_space=pl.ANY)
    heads, rotated = pl.pallas_call(
        body,
        out_shape=(
            jax.ShapeDtypeStruct((KV_HEADS, TOK, PAIR), bf),
            jax.ShapeDtypeStruct((KV_HEADS, TOK, HEAD), bf),
        ),
        in_specs=[anywhere, anywhere, anywhere, smem, smem, anywhere, vmem],
        out_specs=(anywhere, anywhere),
        scratch_shapes=[
            pltpu.VMEM((TOK, 2 * KV_HEADS * HEAD), bf),
            pltpu.VMEM((TOK, KV_HEADS * HEAD), bf),
            pltpu.VMEM((KV_HEADS, TOK, PAIR), bf),
            pltpu.VMEM((KV_HEADS, TOK, HEAD), bf),
            pltpu.VMEM((KV_HEADS, TOK, HEAD), bf),
            pltpu.VMEM((RING, TOK, PAIR), bf),
            pltpu.VMEM((2 * RING * TOK, HEAD), bf),
            pltpu.VMEM((2 * RING * TOK, HEAD), bf),
            pltpu.VMEM((n_batch * pool_rows, PAGE, PAIR), bf),
            pltpu.VMEM((pool_rows, PAGE, PAIR), bf),
            pltpu.VMEM((TOK, PAIR), bf),
            pltpu.VMEM((RING + 2, 2 * TOK, TOK), jnp.float32),
            pltpu.VMEM((2 * TOK, HEAD), bf),
            pltpu.VMEM((RING, TOK, PAIR), bf),
            dma((RING,)),
            dma((RING,)),
            dma((RING,)),
            dma((RING,)),
            dma((RING,)),
            dma((RING,)),
            dma((RING,)),
            dma((RING,)),
            dma((RING,)),
            dma((RING,)),
            dma((n_batch,)),
            dma((n_batch,)),
            dma((RING,)),
            dma((RING,)),
            dma((7,)),
            dma((KV_HEADS,)),
        ],
        compiler_params=pltpu.CompilerParams(
            collective_id=0, has_side_effects=True, vmem_limit_bytes=67043328
        ),
    )(queries, keys, values, lengths, jnp.transpose(page_table, (1, 2, 0)), pool, freq)
    return pl.pallas_call(
        finish,
        out_shape=(
            jax.ShapeDtypeStruct(queries.shape, bf),
            jax.ShapeDtypeStruct(keys.shape, bf),
        ),
        in_specs=[anywhere, anywhere],
        out_specs=(anywhere, anywhere),
        scratch_shapes=[
            pltpu.VMEM((KV_HEADS, TOK, PAIR), bf),
            pltpu.VMEM((KV_HEADS, TOK, HEAD), bf),
            dma((KV_HEADS,)),
            dma((KV_HEADS,)),
            dma((KV_HEADS,)),
            dma((KV_HEADS,)),
        ],
        compiler_params=pltpu.CompilerParams(vmem_limit_bytes=67043328),
    )(heads, rotated)


def solution(mesh):
    in_specs = (
        P("batch", "blk", None),
        P("batch", "blk", None),
        P("batch", "blk", None),
        P("batch", "blk"),
        P("batch", None),
        P("batch", "blk", None),
        P(),
        P("batch", None, None),
    )
    out_specs = (P("batch", "blk", None), P("batch", "blk", None))
    return jax.shard_map(
        per_device, mesh=mesh, in_specs=in_specs, out_specs=out_specs, check_vma=False
    )
```

```python
import math

import jax
import jax.numpy as jnp
import numpy as np
from jax import lax
from jax.experimental import pallas as pl
from jax.experimental.pallas import tpu as pltpu
from jax.sharding import PartitionSpec as P

HEAD = 128
KV_HEADS = 8
RING = 8
TOK = 256
SEGS = 7
PAGES_SEG = 2
PAGE = 16
PREFIX = PAGES_SEG * PAGE
PAIR = 2 * HEAD
ROPE_BASE = 1000000.0
LOG2E_SCALE = math.log2(math.e) / math.sqrt(HEAD)
NEG = -1e30
MESH = pl.DeviceIdType.MESH


def kernel(
    n_x,
    n_batch,
    pool_rows,
    queries,
    keys,
    values,
    lengths,
    page_table,
    pool,
    freq,
    attended,
    cache,
    qraw,
    kraw,
    qrot,
    krot,
    vown,
    qbuf,
    kbuf,
    vbuf,
    pbuf,
    pown,
    pre,
    scores,
    q2,
    obuf,
    v_send,
    v_recv,
    k_send,
    k_recv,
    q_send,
    q_recv,
    fv_send,
    fv_recv,
    fk_send,
    fk_recv,
    p_send,
    p_recv,
    o_send,
    o_recv,
    local,
    v_load,
):
    blk = lax.axis_index("blk")
    bat = lax.axis_index("batch")
    z = lax.rem(blk, RING)
    x = lax.div(blk, RING)

    def ring(d):
        return lax.rem(z + d, RING)

    def ring_id(d):
        return (x * RING + ring(d), bat)

    def other(e):
        return lax.rem(bat + e, n_batch)

    def lanes(i, width):
        return pl.ds(pl.multiple_of(i * width, width), width)

    def rows(i):
        return pl.ds(pl.multiple_of(i * TOK, TOK), TOK)

    ahead = (lax.rem(x + 1, n_x) * RING + z, bat)
    behind = (lax.rem(x + n_x - 1, n_x) * RING + z, bat)

    barrier = pltpu.get_barrier_semaphore()
    for d in range(1, RING):
        pl.semaphore_signal(barrier, inc=1, device_id=ring_id(d), device_id_type=MESH)
    for who in (ahead, behind):
        pl.semaphore_signal(barrier, inc=1, device_id=who, device_id_type=MESH)
    for e in range(1, n_batch):
        pl.semaphore_signal(barrier, inc=1, device_id=(blk, other(e)), device_id_type=MESH)
    own_pool_k = pltpu.make_async_copy(pool.at[:, :, lanes(z, HEAD)], pown.at[:, :, 0:HEAD], local.at[0])
    own_pool_v = pltpu.make_async_copy(
        pool.at[:, :, lanes(z + KV_HEADS, HEAD)], pown.at[:, :, HEAD:PAIR], local.at[1]
    )
    def load_v(d):
        return pltpu.make_async_copy(
            values.at[0, :, lanes(ring(d), HEAD)], vown.at[ring(d)], v_load.at[d]
        )

    order = (4, 3, 5, 2, 6, 1, 7)
    near = (1, 7, 2, 6, 3, 5, 4)
    load_k = pltpu.make_async_copy(keys.at[0], kraw, local.at[5])
    load_q = pltpu.make_async_copy(queries.at[0], qraw, local.at[6])
    for d in near + (0,):
        load_v(d).start()
    load_k.start()
    own_pool_k.start()
    own_pool_v.start()
    load_q.start()
    pl.semaphore_wait(barrier, RING - 1 + 2 + n_batch - 1)

    def send_v(d):
        return pltpu.make_async_remote_copy(
            src_ref=vown.at[ring(d)],
            dst_ref=vbuf.at[rows(RING + z)],
            send_sem=v_send.at[d],
            recv_sem=v_recv.at[d],
            device_id=ring_id(d),
            device_id_type=MESH,
        )

    def send_k(d):
        return pltpu.make_async_remote_copy(
            src_ref=krot.at[ring(d)],
            dst_ref=kbuf.at[rows(RING + z)],
            send_sem=k_send.at[d],
            recv_sem=k_recv.at[d],
            device_id=ring_id(d),
            device_id_type=MESH,
        )

    def send_q(d):
        return pltpu.make_async_remote_copy(
            src_ref=qrot.at[ring(d)],
            dst_ref=qbuf.at[z],
            send_sem=q_send.at[d],
            recv_sem=q_recv.at[d],
            device_id=ring_id(d),
            device_id_type=MESH,
        )

    def send_pool(e):
        return pltpu.make_async_remote_copy(
            src_ref=pown,
            dst_ref=pbuf.at[pl.ds(bat * pool_rows, pool_rows)],
            send_sem=p_send.at[e],
            recv_sem=p_recv.at[e],
            device_id=(blk, other(e)),
            device_id_type=MESH,
        )

    def forward(buf, sends, recvs, s, src=None):
        return pltpu.make_async_remote_copy(
            src_ref=buf.at[rows(RING + s)] if src is None else src,
            dst_ref=buf.at[rows(s)],
            send_sem=sends.at[s],
            recv_sem=recvs.at[s],
            device_id=ahead,
            device_id_type=MESH,
        )

    def forward_v(s, src=None):
        return forward(vbuf, fv_send, fv_recv, s, src)

    def forward_k(s, src=None):
        return forward(kbuf, fk_send, fk_recv, s, src)

    def send_o(d):
        return pltpu.make_async_remote_copy(
            src_ref=obuf.at[d],
            dst_ref=attended.at[z],
            send_sem=o_send.at[d],
            recv_sem=o_recv.at[d],
            device_id=ring_id(RING - d),
            device_id_type=MESH,
        )

    for d in near:
        load_v(d).wait()
        send_v(d).start()
    load_v(0).wait()
    own_v = pltpu.make_async_copy(vown.at[z], vbuf.at[rows(RING + z)], local.at[2])
    own_v.start()
    forward_v(z, vown.at[z]).start()
    own_pool_k.wait()
    own_pool_v.wait()
    for e in range(1, n_batch):
        send_pool(e).start()
    own_pool = pltpu.make_async_copy(pown, pbuf.at[pl.ds(bat * pool_rows, pool_rows)], local.at[0])
    own_pool.start()

    starts = [jnp.int32(0)]
    for s in range(SEGS - 1):
        starts.append(starts[-1] + lengths[0, s])

    def start_and_segment(token):
        first = jnp.zeros_like(token)
        segment = jnp.zeros_like(token)
        for s in range(1, SEGS):
            inside = token >= starts[s]
            first = jnp.where(inside, starts[s], first)
            segment = jnp.where(inside, s, segment)
        return first, segment

    row = lax.broadcasted_iota(jnp.int32, (TOK, HEAD), 0)
    lane = lax.broadcasted_iota(jnp.int32, (TOK, HEAD), 1)
    token = row + blk * TOK
    first, _ = start_and_segment(token)
    angle = (PREFIX + token - first).astype(jnp.float32) * freq[0:1, :]
    cosine = jnp.cos(angle)
    sine = jnp.sin(angle)
    sine = jnp.where(lane < HEAD // 2, -sine, sine)

    def turn(part):
        part = part.astype(jnp.float32)
        return (part * cosine + pltpu.roll(part, HEAD // 2, 1) * sine).astype(jnp.bfloat16)

    load_k.wait()
    for h in range(KV_HEADS):
        krot[h] = turn(kraw[:, h * HEAD : (h + 1) * HEAD])
    for d in near:
        send_k(d).start()
    own_k = pltpu.make_async_copy(krot.at[z], kbuf.at[rows(RING + z)], local.at[1])
    own_k.start()
    forward_k(z, krot.at[z]).start()
    cache_copy = pltpu.make_async_copy(krot, cache, local.at[3])
    cache_copy.start()
    load_q.wait()
    for h in range(2 * KV_HEADS):
        at = (h % 2) * HEAD
        qrot[h // 2, :, at : at + HEAD] = turn(qraw[:, h * HEAD : (h + 1) * HEAD])
    for d in order:
        send_q(d).start()
    own_q = pltpu.make_async_copy(qrot.at[z], qbuf.at[z], local.at[4])
    own_q.start()

    def from_ring(buf, recvs, d):
        view = buf.at[rows(RING + ring(RING - d))]
        return pltpu.make_async_remote_copy(
            src_ref=view,
            dst_ref=view,
            send_sem=v_send.at[d],
            recv_sem=recvs.at[d],
            device_id=ring_id(RING - d),
            device_id_type=MESH,
        )

    for d in near:
        from_ring(vbuf, v_recv, d).wait_recv()
        forward_v(ring(RING - d)).start()
    for d in near:
        from_ring(kbuf, k_recv, d).wait_recv()
        forward_k(ring(RING - d)).start()
    own_v.wait()
    own_k.wait()

    own_pool.wait()
    for e in range(1, n_batch):
        src = pl.ds(lax.rem(bat + n_batch - e, n_batch) * pool_rows, pool_rows)
        pltpu.make_async_remote_copy(
            src_ref=pown,
            dst_ref=pbuf.at[src],
            send_sem=p_send.at[e],
            recv_sem=p_recv.at[e],
            device_id=(blk, other(n_batch - e)),
            device_id_type=MESH,
        ).wait_recv()
    for s in range(SEGS):
        for i in range(PAGES_SEG):
            at = s * PREFIX + i * PAGE
            pre[at : at + PAGE, :] = pbuf[page_table[s, i, bat]]
    pre[SEGS * PREFIX :, :] = jnp.zeros((TOK - SEGS * PREFIX, PAIR), jnp.bfloat16)

    for s in range(RING):
        forward_v(s).wait_recv()
        forward_k(s).wait_recv()

    contract_last = (((1,), (1,)), ((), ()))

    def one_block(i, carry):
        odd = lax.rem(i, 2)
        half = lax.div(i + 1, 2)
        d = RING // 2 + (1 - 2 * odd) * half
        src = ring(RING - d)

        @pl.when(d == 0)
        def _():
            pltpu.make_async_copy(qrot.at[z], qbuf.at[z], local.at[4]).wait()

        @pl.when(d > 0)
        def _():
            pltpu.make_async_remote_copy(
                src_ref=qbuf.at[src],
                dst_ref=qbuf.at[src],
                send_sem=q_send.at[d],
                recv_sem=q_recv.at[d],
                device_id=ring_id(RING - d),
                device_id_type=MESH,
            ).wait_recv()

        q2[0:TOK, :] = qbuf[src, :, 0:HEAD]
        q2[TOK : 2 * TOK, :] = qbuf[src, :, HEAD:PAIR]
        block0 = (x * RING + src) * TOK
        begin, segment = start_and_segment(row + block0)
        limit = begin - lane - (block0 - RING * TOK)
        causal = row - lane
        segment_at = segment * PREFIX - lane
        highest = [jnp.full((TOK, HEAD), NEG, jnp.float32)] * 2
        for c in range(RING + 2):
            if c <= RING:
                tile = kbuf[rows(src + c), :]
            else:
                tile = pre[:, 0:HEAD]
            score = lax.dot_general(
                q2[...], tile, contract_last, preferred_element_type=jnp.float32
            )
            for part in range(2):
                at = part * HEAD
                if c < RING:
                    seen = limit <= c * TOK + at
                elif c == RING:
                    seen = (limit <= c * TOK + at) & (causal >= at)
                else:
                    seen = (segment_at <= at) & (segment_at > at - PREFIX)
                for g in range(2):
                    own = slice(g * TOK, (g + 1) * TOK)
                    piece = jnp.where(seen, score[own, at : at + HEAD], NEG)
                    highest[g] = jnp.maximum(highest[g], piece)
                    scores[c, own, at : at + HEAD] = piece
        top = jnp.concatenate([jnp.max(part, axis=1, keepdims=True) for part in highest], axis=0)
        total = jnp.zeros((2 * TOK, HEAD), jnp.float32)
        summed = jnp.zeros((2 * TOK, HEAD), jnp.float32)
        for c in range(RING + 2):
            weight = jnp.exp2((scores[c] - top) * LOG2E_SCALE)
            total = total + (weight[:, 0:HEAD] + weight[:, HEAD:PAIR])
            if c <= RING:
                tile = vbuf[rows(src + c), :]
            else:
                tile = pre[:, HEAD:PAIR]
            summed = summed + jnp.dot(
                weight.astype(jnp.bfloat16), tile, preferred_element_type=jnp.float32
            )
        result = (summed / jnp.sum(total, axis=1, keepdims=True)).astype(jnp.bfloat16)
        obuf[d, :, 0:HEAD] = result[0:TOK]
        obuf[d, :, HEAD:PAIR] = result[TOK : 2 * TOK]

        @pl.when(d == 0)
        def _():
            pltpu.make_async_copy(
                obuf.at[0], attended.at[z], local.at[2]
            ).start()

        @pl.when(d > 0)
        def _():
            send_o(d).start()

        return carry

    lax.fori_loop(0, RING, one_block, 0)

    for d in range(1, RING):
        send_v(d).wait_send()
        send_k(d).wait_send()
        send_q(d).wait_send()
    for s in range(RING):
        forward_v(s).wait_send()
        forward_k(s).wait_send()
    for e in range(1, n_batch):
        send_pool(e).wait_send()
    cache_copy.wait()
    pltpu.make_async_copy(obuf.at[0], attended.at[z], local.at[2]).wait()
    for d in range(1, RING):
        send_o(d).wait_send()
        pltpu.make_async_remote_copy(
            src_ref=obuf.at[d],
            dst_ref=attended.at[ring(d)],
            send_sem=o_send.at[d],
            recv_sem=o_recv.at[d],
            device_id=ring_id(d),
            device_id_type=MESH,
        ).wait_recv()


def finish(heads, rotated, attended, cache, h_buf, r_buf, h_in, r_in, h_out, r_out):
    loads = []
    for s in range(KV_HEADS):
        loads.append(pltpu.make_async_copy(heads.at[s], h_buf.at[s], h_in.at[s]))
        loads.append(pltpu.make_async_copy(rotated.at[s], r_buf.at[s], r_in.at[s]))
    for copy in loads:
        copy.start()
    stores = []
    for s in range(KV_HEADS):
        stores.append(
            pltpu.make_async_copy(
                h_buf.at[s], attended.at[0, :, s * PAIR : (s + 1) * PAIR], h_out.at[s]
            )
        )
        stores.append(
            pltpu.make_async_copy(
                r_buf.at[s], cache.at[0, :, s * HEAD : (s + 1) * HEAD], r_out.at[s]
            )
        )
    for load, store in zip(loads, stores):
        load.wait()
        store.start()
    for copy in stores:
        copy.wait()


def per_device(queries, keys, values, seg_ids, lengths, live, page_table, pool):
    n_x = lax.axis_size("blk") // RING
    n_batch = lax.axis_size("batch")
    pool_rows = pool.shape[0]
    half = HEAD // 2
    inverse = np.power(np.float64(ROPE_BASE), -2.0 * np.arange(half) / HEAD)
    freq = jnp.asarray(np.tile(np.concatenate([inverse, inverse])[None], (8, 1)), jnp.float32)

    def body(*refs):
        kernel(n_x, n_batch, pool_rows, *refs)

    bf = jnp.bfloat16
    dma = pltpu.SemaphoreType.DMA
    vmem = pl.BlockSpec(memory_space=pltpu.VMEM)
    smem = pl.BlockSpec(memory_space=pltpu.SMEM)
    anywhere = pl.BlockSpec(memory_space=pl.ANY)
    heads, rotated = pl.pallas_call(
        body,
        out_shape=(
            jax.ShapeDtypeStruct((KV_HEADS, TOK, PAIR), bf),
            jax.ShapeDtypeStruct((KV_HEADS, TOK, HEAD), bf),
        ),
        in_specs=[anywhere, anywhere, anywhere, smem, smem, anywhere, vmem],
        out_specs=(anywhere, anywhere),
        scratch_shapes=[
            pltpu.VMEM((TOK, 2 * KV_HEADS * HEAD), bf),
            pltpu.VMEM((TOK, KV_HEADS * HEAD), bf),
            pltpu.VMEM((KV_HEADS, TOK, PAIR), bf),
            pltpu.VMEM((KV_HEADS, TOK, HEAD), bf),
            pltpu.VMEM((KV_HEADS, TOK, HEAD), bf),
            pltpu.VMEM((RING, TOK, PAIR), bf),
            pltpu.VMEM((2 * RING * TOK, HEAD), bf),
            pltpu.VMEM((2 * RING * TOK, HEAD), bf),
            pltpu.VMEM((n_batch * pool_rows, PAGE, PAIR), bf),
            pltpu.VMEM((pool_rows, PAGE, PAIR), bf),
            pltpu.VMEM((TOK, PAIR), bf),
            pltpu.VMEM((RING + 2, 2 * TOK, TOK), jnp.float32),
            pltpu.VMEM((2 * TOK, HEAD), bf),
            pltpu.VMEM((RING, TOK, PAIR), bf),
            dma((RING,)),
            dma((RING,)),
            dma((RING,)),
            dma((RING,)),
            dma((RING,)),
            dma((RING,)),
            dma((RING,)),
            dma((RING,)),
            dma((RING,)),
            dma((RING,)),
            dma((n_batch,)),
            dma((n_batch,)),
            dma((RING,)),
            dma((RING,)),
            dma((7,)),
            dma((KV_HEADS,)),
        ],
        compiler_params=pltpu.CompilerParams(
            collective_id=0, has_side_effects=True, vmem_limit_bytes=67043328
        ),
    )(queries, keys, values, lengths, jnp.transpose(page_table, (1, 2, 0)), pool, freq)
    return pl.pallas_call(
        finish,
        out_shape=(
            jax.ShapeDtypeStruct(queries.shape, bf),
            jax.ShapeDtypeStruct(keys.shape, bf),
        ),
        in_specs=[anywhere, anywhere],
        out_specs=(anywhere, anywhere),
        scratch_shapes=[
            pltpu.VMEM((KV_HEADS, TOK, PAIR), bf),
            pltpu.VMEM((KV_HEADS, TOK, HEAD), bf),
            dma((KV_HEADS,)),
            dma((KV_HEADS,)),
            dma((KV_HEADS,)),
            dma((KV_HEADS,)),
        ],
        compiler_params=pltpu.CompilerParams(vmem_limit_bytes=67043328),
    )(heads, rotated)


def solution(mesh):
    in_specs = (
        P("batch", "blk", None),
        P("batch", "blk", None),
        P("batch", "blk", None),
        P("batch", "blk"),
        P("batch", None),
        P("batch", "blk", None),
        P(),
        P("batch", None, None),
    )
    out_specs = (P("batch", "blk", None), P("batch", "blk", None))
    return jax.shard_map(
        per_device, mesh=mesh, in_specs=in_specs, out_specs=out_specs, check_vma=False
    )
```
